32 devices in a mesh: gx: 4 (over z), gy: 4 (over y, x), gz: 2 (over core).
Axes of the slice: x: 2, y: 2, z: 4, core: 2. Of those that a mesh axis runs over, the one named last changes fastest.
Arguments:
- source_points: float32 [3, 13, 4, 16, 4, 512], P(None, None, 'gx', 'gy', 'gz'), may hold values from -3 to 3
- target_points: float32 [3, 13, 4, 16, 4, 512], P(None, None, 'gx', 'gy', 'gz'), may hold values from -3 to 3
- normals: float32 [3, 13, 4, 16, 4, 512], P(None, None, 'gx', 'gy', 'gz'), may hold values from -4 to 4
- weights: float32 [13, 4, 16, 4, 512], P(None, 'gx', 'gy', 'gz'), may hold values from 0.1 to 1
- blocks: int32 [13, 4, 16, 4], P(None, 'gx', 'gy', 'gz'), may hold values from 0 to 2
- affines: float32 [12, 4, 16, 4], P(None, 'gx', 'gy', 'gz'), may hold values from -0.5 to 0.5
- anchor: int32 [1], replicated, may hold values from 0 to 255
Outputs:
- update: float32 [12, 4, 16, 4], P(None, 'gx', 'gy', 'gz')
- residual: float32 [12, 4, 16, 4], P(None, 'gx', 'gy', 'gz')
The draws below stay inside these ranges and needn't reach their ends.
Inputs may be any that keep to these rules, and one draw needn't show every extreme that they name: `blocks`: number of 256-point correspondence blocks of the correlation; entries of correlations whose second tile lies outside the grid are not read. `anchor`: a tile index (x 16 + y) * 4 + z.
All inputs are finite; a program needn't handle non-finite values.
Results may differ from the reference program's by a relative error of at most 0.0003.
Values sent between devices are 32-bit elements; how exact they have to be, the bound alone decides.
A program may use at most 128 MiB of HBM per device.

```python
import math
import jax
import jax.numpy as jnp
from jax import lax

DIRS = 13
BLOCK = 256
MAXB = 2
ITERS = 10
PTS = 512
NX = 4
NY = 16
NZ = 4


def touch_ends(drawn, stream_key, low, largest):
    index_at = [jax.random.randint(jax.random.fold_in(stream_key, axis), (), 0, length) for axis, length in enumerate(drawn.shape)]
    widest = drawn.shape.index(max(drawn.shape))
    next_to = index_at[:widest] + [(index_at[widest] + 1) % drawn.shape[widest]] + index_at[widest + 1:]
    return drawn.at[tuple(index_at)].set(low).at[tuple(next_to)].set(largest)


def steps_of(key, shape, pieces, smallest, largest):
    loudness, own = 1.0, jax.random.fold_in(key, 6)
    for dim, parts in pieces:
        draws = jnp.exp(jax.random.uniform(jax.random.fold_in(own, dim), (parts,), jnp.float32, smallest / len(pieces), largest / len(pieces)))
        loudness = loudness * jnp.repeat(draws, shape[dim] // parts).reshape([-1 if axis == dim else 1 for axis in range(len(shape))])
    return loudness


def centred(own_key, dims, scale, most, pieces=(), kind=jnp.bfloat16):
    factor_of = steps_of(own_key, dims, pieces, -0.22, 0.18) if pieces else 1.0
    array = jax.random.normal(own_key, dims, jnp.float32) * scale * factor_of
    return jnp.minimum(jnp.maximum(array, -most), most).astype(kind)


def setup_inputs(seed: int = 0) -> dict:
    keys = jax.random.split(jax.random.key(seed), 8)
    return {
        "source_points": centred(keys[0], (3, DIRS, NX, NY, NZ, PTS), 0.5, 3.0, ((2, 4), (3, 4), (4, 2)), jnp.float32),
        "target_points": centred(keys[1], (3, DIRS, NX, NY, NZ, PTS), 0.5, 3.0, ((2, 4), (3, 4), (4, 2)), jnp.float32),
        "normals": centred(keys[2], (3, DIRS, NX, NY, NZ, PTS), 1.0, 4.0, ((2, 4), (3, 4), (4, 2)), jnp.float32),
        "weights": jnp.clip(jnp.exp(math.log(1.0) - 2.3025851 * jax.random.uniform(keys[3], (DIRS, NX, NY, NZ, PTS), jnp.float32) ** steps_of(keys[3], (DIRS, NX, NY, NZ, PTS), ((1, 4), (2, 4), (3, 2)), -0.2, 0.2)), 0.1, 1.0),
        "blocks": touch_ends(jax.random.randint(keys[4], (DIRS, NX, NY, NZ), 0, MAXB + 1), jax.random.fold_in(keys[4], 1), 0, MAXB).astype(jnp.int32),
        "affines": centred(keys[5], (12, NX, NY, NZ), 0.1, 0.5, ((1, 4), (2, 4), (3, 2)), jnp.float32),
        "anchor": jax.random.randint(keys[6], (1,), 0, NX * NY * NZ).astype(jnp.int32),
    }


SPACING = 0.5
DAMPING = 1.0
OFFSETS = ((1, 0, 0), (0, 1, 0), (0, 0, 1), (1, 1, -1), (1, -1, 1), (-1, 1, 1), (1, 1, 0), (1, 0, 1), (0, 1, 1), (1, 1, 1), (1, -1, 0), (0, 1, -1), (-1, 0, 1))


def negated(offset):
    return tuple(-part for part in offset)


def moved(values, offset, first):
    widths = [(0, 0)] * values.ndim
    for axis in range(3):
        widths[first + axis] = (1, 1)
    padded = jnp.pad(values, widths)
    picks = [slice(None)] * values.ndim
    for axis in range(3):
        length = values.shape[first + axis]
        picks[first + axis] = slice(1 + offset[axis], 1 + offset[axis] + length)
    return padded[tuple(picks)]


def lifted(points):
    return jnp.concatenate([points, jnp.ones((1,) + points.shape[1:], points.dtype)], axis=0)


def mapped(affine, lifted_points):
    matrix = affine.reshape((3, 4) + affine.shape[1:]) + jnp.eye(3, 4, dtype=affine.dtype).reshape(3, 4, 1, 1, 1)
    return jnp.einsum("cexyz,exyzp->cxyzp", matrix, lifted_points, precision=lax.Precision.HIGHEST)


def correlation_terms(source, target, normal, weight, affine_here, affine_there, offset):
    exact = lax.Precision.HIGHEST
    source_lift = lifted(source)
    target_lift = lifted(target)
    stride = jnp.asarray(offset, source.dtype).reshape(3, 1, 1, 1, 1) * SPACING
    misfit = jnp.sum(normal * (mapped(affine_here, source_lift) - mapped(affine_there, target_lift) - stride), axis=0)
    layout = (12,) + source.shape[1:]
    rows_here = (normal[:, None] * source_lift[None]).reshape(layout)
    rows_there = -(normal[:, None] * target_lift[None]).reshape(layout)
    weighted_here = rows_here * weight
    weighted_there = rows_there * weight
    block_here = jnp.einsum("axyzp,bxyzp->abxyz", weighted_here, rows_here, precision=exact)
    block_pair = jnp.einsum("axyzp,bxyzp->abxyz", weighted_here, rows_there, precision=exact)
    block_there = jnp.einsum("axyzp,bxyzp->abxyz", weighted_there, rows_there, precision=exact)
    pull_here = jnp.einsum("axyzp,xyzp->axyz", weighted_here, misfit, precision=exact)
    pull_there = jnp.einsum("axyzp,xyzp->axyz", weighted_there, misfit, precision=exact)
    return block_here, block_pair, block_there, pull_here, pull_there


def invert_blocks(blocks):
    left = blocks
    right = jnp.broadcast_to(jnp.eye(12, dtype=blocks.dtype).reshape((12, 12) + (1,) * (blocks.ndim - 2)), blocks.shape)
    for pivot in range(12):
        factor = 1.0 / left[pivot, pivot]
        row_left = left[pivot] * factor
        row_right = right[pivot] * factor
        column = left[:, pivot]
        left = left - column[:, None] * row_left[None]
        right = right - column[:, None] * row_right[None]
        left = left.at[pivot].set(row_left)
        right = right.at[pivot].set(row_right)
    return right


def reference(source_points, target_points, normals, weights, blocks, affines, anchor):
    exact = lax.Precision.HIGHEST
    grid_x = jnp.arange(NX, dtype=jnp.int32).reshape(NX, 1, 1)
    grid_y = jnp.arange(NY, dtype=jnp.int32).reshape(1, NY, 1)
    grid_z = jnp.arange(NZ, dtype=jnp.int32).reshape(1, 1, NZ)
    flat = (grid_x * NY + grid_y) * NZ + grid_z
    keep = (flat != anchor[0]).astype(jnp.float32)
    filled = jnp.ones((NX, NY, NZ), jnp.float32)
    slots = jnp.arange(PTS, dtype=jnp.int32).reshape(1, 1, 1, PTS)
    diag = jnp.zeros((12, 12, NX, NY, NZ), jnp.float32)
    pull = jnp.zeros((12, NX, NY, NZ), jnp.float32)
    pairs = []
    for index, offset in enumerate(OFFSETS):
        inside = moved(filled, offset, 0)
        live = (slots < BLOCK * blocks[index][..., None]).astype(jnp.float32) * inside[..., None]
        target = moved(target_points[:, index], offset, 1)
        affine_there = moved(affines, offset, 1)
        block_here, block_pair, block_there, pull_here, pull_there = correlation_terms(
            source_points[:, index], target, normals[:, index], weights[index] * live, affines, affine_there, offset)
        diag = diag + block_here + moved(block_there, negated(offset), 2)
        pull = pull + pull_here + moved(pull_there, negated(offset), 1)
        pairs.append(block_pair * (keep * moved(keep, offset, 0)))
    coupling = jnp.stack(pairs)
    identity = jnp.eye(12, dtype=jnp.float32).reshape(12, 12, 1, 1, 1)
    diag = keep * (diag + DAMPING * identity) + (1.0 - keep) * identity
    rhs = -(keep * pull)
    inverse = invert_blocks(diag)

    def operate(vector):
        result = jnp.einsum("abxyz,bxyz->axyz", diag, vector, precision=exact)
        for index, offset in enumerate(OFFSETS):
            result = result + jnp.einsum("abxyz,bxyz->axyz", coupling[index], moved(vector, offset, 1), precision=exact)
            sent = jnp.einsum("baxyz,bxyz->axyz", coupling[index], vector, precision=exact)
            result = result + moved(sent, negated(offset), 1)
        return result

    def precondition(vector):
        return jnp.einsum("abxyz,bxyz->axyz", inverse, vector, precision=exact)

    update = jnp.zeros_like(rhs)
    residual = rhs
    scaled = precondition(residual)
    direction = scaled
    inner = jnp.sum(residual * scaled)
    for step in range(ITERS):
        image = operate(direction)
        alpha = inner / jnp.sum(direction * image)
        update = update + alpha * direction
        residual = residual - alpha * image
        scaled = precondition(residual)
        inner_next = jnp.sum(residual * scaled)
        direction = scaled + (inner_next / inner) * direction
        inner = inner_next
    return update, residual
```

```python
import functools

import jax
import jax.numpy as jnp
from jax import lax
from jax.experimental import pallas as pl
from jax.experimental.pallas import tpu as pltpu
from jax.sharding import PartitionSpec as P

BLOCK = 256
ITERS = 10
SPACING = 0.5
DAMPING = 1.0
OFFSETS = (
    (1, 0, 0),
    (0, 1, 0),
    (0, 0, 1),
    (1, 1, -1),
    (1, -1, 1),
    (-1, 1, 1),
    (1, 1, 0),
    (1, 0, 1),
    (0, 1, 1),
    (1, 1, 1),
    (1, -1, 0),
    (0, 1, -1),
    (-1, 0, 1),
)
DIRS = len(OFFSETS)
LANES = 128
AXES = ("gx", "gy", "gz")
MESH = pl.DeviceIdType.MESH
VMEM_BYTES = 60 * 1024 * 1024

NORMAL_PAIRS = [(c, k) for c in range(3) for k in range(c, 3)]
POINT_PAIRS = [(e, k) for e in range(3) for k in range(e, 3)]
PAIR_ROWS = 96
THERE_ROWS = 36
SPILL = PAIR_ROWS + THERE_ROWS - LANES
SUMS = PAIR_ROWS + 2 * THERE_ROWS
SPILL_LANE = SPILL + THERE_ROWS
AFFINE_LANE = SPILL_LANE + SPILL * DIRS
SEND_ORDER = (3, 4, 5, 9, 7, 12, 0, 6, 10, 8, 11, 1, 2)
GROUPS = ((1, 2, 8, 11), (3, 4, 5, 9), (7, 12, 0, 6), (10,))


def normal_pair(c, k):
    return NORMAL_PAIRS.index((min(c, k), max(c, k)))


def point_pair(e, k):
    return POINT_PAIRS.index((min(e, k), max(e, k)))


def moves(step, length):
    if step == 0:
        return [(slice(0, length), slice(0, length), 0)]
    if step > 0:
        return [
            (slice(step, length), slice(0, length - step), 0),
            (slice(0, step), slice(length - step, length), -1),
        ]
    return [
        (slice(0, length + step), slice(-step, length), 0),
        (slice(length + step, length), slice(0, -step), 1),
    ]


def halo_pieces(bricks):
    pieces = []
    for d in SEND_ORDER:
        dx, dy, dz = OFFSETS[d]
        for y_from, y_to, y_step in moves(dy, bricks[1]):
            for z_from, z_to, z_step in moves(dz, bricks[2]):
                pieces.append((d, (y_from, z_from), (y_to, z_to), (-dx, y_step, z_step)))
    return pieces


def all_of(conditions):
    result = None
    for condition in conditions:
        result = condition if result is None else jnp.logical_and(result, condition)
    return result


def assemble_kernel(
    devices, bricks,
    count, affine, source, target, normal, weight,
    out,
    own_p, own_n, own_w, there, turned, acc,
    load_sem, stay_sem, halo_send, halo_recv,
    line_send, line_recv, side_send, side_recv, far_recv, core_send, core_recv,
):
    count_x, count_y, count_z = devices
    _, side_y, side_z = bricks
    at = tuple(lax.axis_index(name) for name in AXES)
    at_x, at_y, at_z = at
    pieces = halo_pieces(bricks)
    chunks = source.shape[3] // side_z

    def in_mesh(offset):
        return all_of(
            [
                (at[axis] + step >= 0) & (at[axis] + step < devices[axis])
                for axis, step in enumerate(offset)
                if step
            ]
        )

    def beside(offset):
        return tuple(
            jnp.clip(at[axis] + step, 0, devices[axis] - 1) if step else at[axis]
            for axis, step in enumerate(offset)
        )

    near_y = (at_y + 1 - 2 * (at_y % 2), (at_y + 2) % count_y)

    loads = []
    for g, group in enumerate(GROUPS):
        for d in group:
            loads.append(
                (
                    pltpu.make_async_copy(source.at[:, d], own_p.at[:, d], load_sem.at[0, d]),
                    pltpu.make_async_copy(normal.at[:, d], own_n.at[:, d], load_sem.at[1, d]),
                    pltpu.make_async_copy(weight.at[d], own_w.at[d], load_sem.at[2, d]),
                )
            )
            for copy in loads[-1]:
                copy.start()
    loads = dict(zip([d for group in GROUPS for d in group], loads))

    zeros = jnp.zeros(there.shape[2:], jnp.float32)
    for c in range(3):
        for d in range(DIRS):
            there[c, d] = zeros

    barrier = pltpu.get_barrier_semaphore()
    steps = {piece[3] for piece in pieces if any(piece[3])}
    steps |= {tuple(-s for s in step) for step in steps}
    steps |= {(1, 0, 0), (-1, 0, 0)}
    steps = sorted(steps)
    expected = 0
    for step in steps:
        there_is = in_mesh(step)

        @pl.when(there_is)
        def _(step=step):
            pl.semaphore_signal(barrier, inc=1, device_id=beside(step), device_id_type=MESH)

        expected = expected + there_is.astype(jnp.int32)
    for other in near_y:
        pl.semaphore_signal(barrier, inc=1, device_id=(at_x, other, at_z), device_id_type=MESH)
    for k in range(1, count_z):
        pl.semaphore_signal(
            barrier, inc=1, device_id=(at_x, at_y, (at_z + k) % count_z), device_id_type=MESH
        )
    pl.semaphore_wait(barrier, expected + (2 + count_z - 1))

    def spot(ref, d, where):
        return ref.at[:, d, where[0], :, where[1], :]

    def halo(i):
        d, start, end, step = pieces[i]
        return pltpu.make_async_remote_copy(
            src_ref=spot(target, d, start),
            dst_ref=spot(there, d, end),
            send_sem=halo_send.at[i],
            recv_sem=halo_recv.at[i],
            device_id=beside(step),
            device_id_type=MESH,
        )

    def stay(i):
        d, start, end, _ = pieces[i]
        return pltpu.make_async_copy(spot(target, d, start), spot(there, d, end), stay_sem.at[i])

    for i, piece in enumerate(pieces):
        if any(piece[3]):

            @pl.when(in_mesh(piece[3]))
            def _(i=i):
                halo(i).start()

        else:
            stay(i).start()

    inside = {}
    for axis in range(3):
        length = devices[axis] * bricks[axis]
        for place in range(bricks[axis]):
            for step in (-1, 1):
                ahead = at[axis] * bricks[axis] + place + step
                inside[axis, place, step] = ((ahead >= 0) & (ahead < length)).astype(jnp.int32)

    rows = chunks * side_z
    sub = lax.broadcasted_iota(jnp.int32, (rows, LANES), 0)
    lane = lax.broadcasted_iota(jnp.int32, (rows, LANES), 1)
    point = lane + LANES * (sub // side_z)

    def live_weight(d, y):
        limit = None
        for z in range(side_z):
            value = count[y, z, d] * BLOCK
            for axis, place in enumerate((0, y, z)):
                if OFFSETS[d][axis]:
                    value = value * inside[axis, place, OFFSETS[d][axis]]
            limit = value if limit is None else jnp.where(sub % side_z == z, value, limit)
        return jnp.where(point < limit, own_w[d, y], 0.0)

    def turn(parts):
        missing = LANES - rows * len(parts)
        if missing:
            parts = parts + [jnp.zeros((missing, LANES), jnp.float32)]
        return jnp.concatenate(parts, axis=0).T

    step = 32

    def summed(g, kinds):
        def body(chunk, carry):
            spots = pl.ds(pl.multiple_of(chunk * step, step), step)
            p = [turned[c, g, spots, :] for c in range(3)] + [None]
            q = [turned[7 + c, g, spots, :] for c in range(3)] + [None] if kinds == "there" else None
            n = [turned[3 + c, g, spots, :] for c in range(3)]
            w = turned[6, g, spots, :]

            def times(left, right):
                if left is None:
                    return right
                return left if right is None else left * right

            def add(row, value):
                acc[g, row] += jnp.sum(value.reshape(step // 8, 8, LANES), axis=0)

            wn = [w * n[c] for c in range(3)]
            weighted = [wn[c] * n[k] for c, k in NORMAL_PAIRS]
            if kinds == "here":
                for e in range(4):
                    for s in range(6):
                        add(s * 16 + e * 4 + 3, times(weighted[s], p[e]))
                for place, (e, k) in enumerate(POINT_PAIRS):
                    product = p[e] * p[k]
                    for s in range(6):
                        add(PAIR_ROWS + THERE_ROWS + s * 6 + place, weighted[s] * product)
            else:
                for e in range(4):
                    for k in range(3):
                        product = times(p[e], q[k])
                        for s in range(6):
                            add(s * 16 + e * 4 + k, weighted[s] * product)
                for place, (e, k) in enumerate(POINT_PAIRS):
                    product = q[e] * q[k]
                    for s in range(6):
                        add(PAIR_ROWS + s * 6 + place, weighted[s] * product)
            return carry

        lax.fori_loop(0, LANES // step, body, 0)

    acc[...] = jnp.zeros_like(acc)
    for g, group in enumerate(GROUPS):
        for d in group:
            for copy in loads[d]:
                copy.wait()
        for c in range(3):
            turned[c, g] = turn([own_p[c, d, y] for d in group for y in range(side_y)])
            turned[3 + c, g] = turn([own_n[c, d, y] for d in group for y in range(side_y)])
        turned[6, g] = turn([live_weight(d, y) for d in group for y in range(side_y)])
        summed(g, "here")

    there_rows = there.reshape(3, DIRS, side_y, rows, LANES)
    last = [None] * side_y
    for g, group in enumerate(GROUPS):
        for i, piece in enumerate(pieces):
            if piece[0] in group:
                if any(piece[3]):

                    @pl.when(in_mesh(tuple(-s for s in piece[3])))
                    def _(i=i):
                        halo(i).wait_recv()

                else:
                    stay(i).wait()
        for c in range(3):
            turned[7 + c, g] = turn([there_rows[c, d, y] for d in group for y in range(side_y)])
        summed(g, "there")
        whole = [jnp.sum(acc[g, r : r + 8], axis=1) for r in range(0, SUMS, 8)]
        main = jnp.concatenate(whole[: LANES // 8], axis=0).T
        rest = whole[LANES // 8 :] + [jnp.zeros((2 * LANES - SUMS, LANES), jnp.float32)]
        rest = jnp.concatenate(rest, axis=0).T

        def all_chunks(value):
            span = rows // 2
            while span >= side_z:
                value = value + pltpu.roll(value, span, 0)
                span //= 2
            return value

        for place, d in enumerate(group):
            for y in range(side_y):
                first = (place * side_y + y) * rows
                value = all_chunks(main[first : first + rows])
                out[d, at_x, at_y * side_y + y, at_z] = value[:side_z]
                value = all_chunks(rest[first : first + rows])
                spill = pltpu.roll(jnp.where(lane < SPILL, value, 0.0), SPILL_LANE + SPILL * d, 1)
                value = jnp.where(lane < SPILL, 0.0, value) + spill
                last[y] = value if last[y] is None else last[y] + value
    for y in range(side_y):
        pad = [jnp.zeros((side_z, AFFINE_LANE), jnp.float32), affine[y]]
        pad.append(jnp.zeros((side_z, LANES - AFFINE_LANE - affine.shape[2]), jnp.float32))
        out[DIRS, at_x, at_y * side_y + y, at_z] = last[y][:side_z] + jnp.concatenate(pad, axis=1)

    def part(x, y, z):
        return out.at[:, x, pl.ds(y * side_y, side_y), z]

    def send(x, y, z, send_sem, recv_sem, other):
        return pltpu.make_async_remote_copy(
            src_ref=part(x, y, z),
            dst_ref=part(x, y, z),
            send_sem=send_sem,
            recv_sem=recv_sem,
            device_id=other,
            device_id_type=MESH,
        )

    def along(x, sign):
        other = (jnp.clip(at_x + sign, 0, count_x - 1), at_y, at_z)
        return send(x, at_y, at_z, line_send.at[(sign + 1) // 2, x], line_recv.at[x], other)

    def across(x, way):
        other = (at_x, near_y[way], at_z)
        return send(x, at_y, at_z, side_send.at[way, x], side_recv.at[way, x], other)

    def across_in(x, way):
        other = (at_x, near_y[way], at_z)
        return send(x, near_y[way], at_z, side_send.at[way, x], side_recv.at[way, x], other)

    far_y = (near_y[0] + 2) % count_y

    def far_out(x, way):
        other = (at_x, near_y[1 - way], at_z)
        return send(x, near_y[way], at_z, side_send.at[2 + way, x], far_recv.at[x], other)

    def far_in(x):
        other = (at_x, near_y[0], at_z)
        return send(x, far_y, at_z, side_send.at[2, x], far_recv.at[x], other)

    def core_out(x, y, k):
        other = (at_x, at_y, (at_z + k) % count_z)
        return send(x, y, at_z, core_send.at[k - 1, x, y], core_recv.at[k - 1, x, y], other)

    def core_in(x, y, k):
        from_z = (at_z + count_z - k) % count_z
        other = (at_x, at_y, from_z)
        return send(x, y, from_z, core_send.at[k - 1, x, y], core_recv.at[k - 1, x, y], other)

    def to_cores(x, y):
        for k in range(1, count_z):
            core_out(x, y, k).start()

    def spread(x):
        across(x, 0).start()
        across(x, 1).start()
        to_cores(x, at_y)

    def arrived_side(x):
        for way in range(2):
            across_in(x, way).wait_recv()

            @pl.when(x % 2 == way)
            def _(way=way):
                far_out(x, way).start()

            to_cores(x, near_y[way])

    def arrived_far(x):
        far_in(x).wait_recv()
        to_cores(x, far_y)

    def both_ways(distance, body):
        if distance == 0:
            body(at_x, 0)
            return

        @pl.when(at_x - distance >= 0)
        def _():
            body(at_x - distance, 1)

        @pl.when(at_x + distance < count_x)
        def _():
            body(at_x + distance, -1)

    def own_out(sign):
        @pl.when((at_x + sign >= 0) & (at_x + sign < count_x))
        def _():
            along(at_x, sign).start()

    own_out(1)
    own_out(-1)
    spread(at_x)

    def line_arrived(x, sign):
        along(x, sign).wait_recv()

        @pl.when((at_x + sign >= 0) & (at_x + sign < count_x))
        def _():
            along(x, sign).start()

        spread(x)

    for distance in range(1, count_x + 2):
        if distance < count_x:
            both_ways(distance, line_arrived)
        if 0 <= distance - 1 < count_x:
            both_ways(distance - 1, lambda x, sign: arrived_side(x))
        if 0 <= distance - 2 < count_x:
            both_ways(distance - 2, lambda x, sign: arrived_far(x))

    def finish(x, carry):
        for sign in (1, -1):
            sent = (at_x + sign >= 0) & (at_x + sign < count_x)
            sent = sent & ((x <= at_x) if sign > 0 else (x >= at_x))

            @pl.when(sent)
            def _(sign=sign):
                along(x, sign).wait_send()

        for way in range(2):
            across(x, way).wait_send()

            @pl.when(x % 2 == way)
            def _(way=way):
                far_out(x, way).wait_send()

        def cores(y, inner):
            for k in range(1, count_z):
                core_in(x, y, k).wait_recv()
                core_out(x, y, k).wait_send()
            return inner

        lax.fori_loop(0, count_y, cores, 0)
        return carry

    lax.fori_loop(0, count_x, finish, 0)
    for i, piece in enumerate(pieces):
        if any(piece[3]):

            @pl.when(in_mesh(piece[3]))
            def _(i=i):
                halo(i).wait_send()


def solve_kernel(grid, bricks, anchor, parts, update_out, residual_out, blocks, turned, tiles):
    count_x, count_y, count_z = grid
    _, side_y, side_z = bricks
    half = blocks.shape[3]
    plane = count_y * count_z
    lane = lax.broadcasted_iota(jnp.int32, (8, half), 1)
    sub = lax.broadcasted_iota(jnp.int32, (8, half), 0)
    column = sub % 4
    low = sub < 4

    for r in range(DIRS + 1):
        for start in range(0, half, LANES):
            spots = pl.ds(start, LANES)
            first = parts[r, pl.ds(start, LANES), :].T
            second = parts[r, pl.ds(half + start, LANES), :].T
            for i in range(LANES // 4):
                blocks[r, i, :, spots] = jnp.concatenate(
                    [first[4 * i : 4 * i + 4], second[4 * i : 4 * i + 4]], axis=0
                )

    def ahead(value, offset, sign=1):
        shift = sign * (offset[0] * plane + offset[1] * count_z + offset[2])
        result = pltpu.roll(value, (-shift) % half, 1)
        if offset[0]:
            stays = (lane + shift >= 0) & (lane + shift < half)
            result = jnp.where(stays, result, pltpu.roll(result, 4, 0))
        return result

    def spread(value, e):
        return jnp.where(low, value[e : e + 1], value[4 + e : 5 + e])

    def butterfly(first, second, span):
        takes_first = (column & span) == 0
        return jnp.where(takes_first, first, pltpu.roll(second, span, 0)) + jnp.where(
            takes_first, pltpu.roll(first, 8 - span, 0), second
        )

    def columns_summed(four):
        return butterfly(butterfly(four[0], four[1], 1), butterfly(four[2], four[3], 1), 2)

    def total(terms):
        terms = list(terms)
        while len(terms) > 1:
            terms = [
                terms[i] + terms[i + 1] if i + 1 < len(terms) else terms[i]
                for i in range(0, len(terms), 2)
            ]
        return terms[0]

    def transposed(d, spreads):
        return [
            total(
                blocks[d, normal_pair(c, k) * 4 + e] * spreads[c][e]
                for c in range(3)
                for e in range(4)
            )
            for k in range(3)
        ]

    def operate(vector, shifted=False):
        spreads = [[spread(vector[c], e) for e in range(4)] for c in range(3)]
        result = transposed(DIRS, spreads)
        sums = [[None] * 4 for _ in range(3)]
        back = [None] * 3
        for d, offset in enumerate(OFFSETS):
            near = [ahead(vector[k], offset) for k in range(3)]
            here = spreads
            if shifted:
                near = [
                    near[k] + jnp.where(column == 3, SPACING * offset[k], 0.0) for k in range(3)
                ]
                here = [
                    spreads[c][:3] + [spreads[c][3] - SPACING * offset[c]] for c in range(3)
                ]
            sent = transposed(d, here)
            for c in range(3):
                for e in range(4):
                    term = total(
                        blocks[d, normal_pair(c, k) * 4 + e] * near[k] for k in range(3)
                    )
                    sums[c][e] = term if sums[c][e] is None else sums[c][e] + term
            for k in range(3):
                term = ahead(sent[k], offset, -1)
                back[k] = term if back[k] is None else back[k] + term
        return [result[k] - back[k] - columns_summed(sums[k]) for k in range(3)]

    def rows_of(value):
        return [jnp.concatenate([value[f : f + 1], value[4 + f : 5 + f]], axis=0) for f in range(4)]

    both = []
    for g in range(THERE_ROWS // 4):
        value = blocks[DIRS, SPILL // 4 + g]
        for d, offset in enumerate(OFFSETS):
            group = PAIR_ROWS // 4 + g
            if group < LANES // 4:
                term = blocks[d, group]
            else:
                term = blocks[DIRS, SPILL_LANE // 4 + d]
            value = value + ahead(term, offset, -1)
        both.append(value)
    unit = [(column == k).astype(jnp.float32) for k in range(3)]
    affine = [blocks[DIRS, AFFINE_LANE // 4 + k] + unit[k] for k in range(3)]
    diagonal = []
    for s in range(6):
        edge = None
        for d, offset in enumerate(OFFSETS):
            term = ahead(blocks[d, s * 4 + 3], offset, -1)
            edge = term if edge is None else edge + term
        for e in range(4):
            term = total(blocks[d, s * 4 + e] for d in range(DIRS))
            edge = edge + jnp.where(column == e, spread(term, 3), 0.0)
        for e in range(3):
            value = spread(edge, e)
            for f in range(3):
                i = s * 6 + point_pair(e, f)
                value = jnp.where(column == f, spread(both[i // 4], i % 4), value)
            diagonal.append(value)
        diagonal.append(edge)
    for i, value in enumerate(diagonal):
        blocks[DIRS, i] = value

    flat = lane + jnp.where(low, 0, half)
    keep = (flat != anchor[0]).astype(jnp.float32)
    rhs = [-(keep * value) for value in operate(affine, True)]

    matrix = []
    for c in range(3):
        for e in range(4):
            row = []
            for k in range(3):
                value = blocks[DIRS, normal_pair(c, k) * 4 + e]
                if c == k:
                    eye = (column == e).astype(jnp.float32)
                    damped = value + DAMPING * eye
                    blocks_value = keep * damped + (1.0 - keep) * eye
                else:
                    blocks_value = keep * value
                row.append(blocks_value)
            matrix.append(row)
    for s, (c, k) in enumerate(NORMAL_PAIRS):
        if c == k:
            for e in range(4):
                value = blocks[DIRS, s * 4 + e]
                blocks[DIRS, s * 4 + e] = value + DAMPING * (column == e).astype(jnp.float32)
    for pivot in range(12):
        c, e = divmod(pivot, 4)
        here = matrix[pivot]
        factor = 1.0 / spread(here[c], e)
        at_pivot = column == e
        scaled = [here[k] * factor for k in range(3)]
        scaled[c] = jnp.where(at_pivot, factor, scaled[c])
        for a in range(12):
            if a == pivot:
                matrix[a] = scaled
            else:
                row = list(matrix[a])
                entry = spread(row[c], e)
                row[c] = jnp.where(at_pivot, 0.0, row[c])
                matrix[a] = [row[k] - entry * scaled[k] for k in range(3)]
    for a in range(12):
        for k in range(3):
            turned[a * 3 + k] = matrix[a][k]

    def precondition(vector):
        spreads = [[spread(vector[c], e) for e in range(4)] for c in range(3)]
        return [
            total(
                turned[(4 * c + e) * 3 + k] * spreads[c][e] for c in range(3) for e in range(4)
            )
            for k in range(3)
        ]

    def dot(left, right):
        return jnp.sum(total(left[k] * right[k] for k in range(3)), keepdims=True)

    first = precondition(rhs)

    def step(_, carry):
        update, residual, direction, inner_now = carry
        along = [keep * value for value in operate(direction)]
        alpha = inner_now / dot(direction, along)
        update = [update[k] + alpha * direction[k] for k in range(3)]
        residual = [residual[k] - alpha * along[k] for k in range(3)]
        scaled = precondition(residual)
        inner_next = dot(residual, scaled)
        beta = inner_next / inner_now
        direction = [scaled[k] + beta * direction[k] for k in range(3)]
        return update, residual, direction, inner_next

    start = ([jnp.zeros_like(value) for value in rhs], rhs, first, dot(rhs, first))
    update, residual, _, _ = lax.fori_loop(0, ITERS, step, start)

    at_x, at_y, at_z = (lax.axis_index(name) for name in AXES)
    upper = at_x // (count_x // 2)
    base = (at_x - upper * (count_x // 2)) * plane + at_y * side_y * count_z + at_z * side_z
    chosen = [jnp.where(upper == 0, v[:4], v[4:]) for v in update + residual]
    chosen.append(jnp.zeros((LANES - 24, half), jnp.float32))
    tall = jnp.concatenate(chosen, axis=0)
    for start in range(0, half, LANES):
        tiles[pl.ds(start, LANES), :] = tall[:, start : start + LANES].T
    for y in range(side_y):
        rows = tiles[pl.ds(base + y * count_z, side_z), :]
        update_out[y] = rows[:, :12]
        residual_out[y] = rows[:, 12:24]


def on_device(source_points, target_points, normals, weights, blocks, affines, anchor):
    bricks = source_points.shape[2:5]
    points = source_points.shape[5]
    devices = tuple(lax.axis_size(name) for name in AXES)
    grid = tuple(devices[axis] * bricks[axis] for axis in range(3))
    span = grid[0] * grid[1] * grid[2]
    chunks = points // LANES
    rows = chunks * bricks[2]
    assert bricks[0] == 1 and rows == 8 and grid[0] % 2 == 0 and devices[1] == 4
    assert span % (2 * LANES) == 0 and len(GROUPS[0]) * bricks[1] * rows == LANES

    def split(value):
        lead = value.shape[:-5]
        value = value.reshape(lead + (DIRS, bricks[1], bricks[2], chunks, LANES))
        return jnp.swapaxes(value, -3, -2)

    def filled(value):
        value = split(value)
        return value.reshape(value.shape[:-3] + (rows, LANES))

    params = functools.partial(pltpu.CompilerParams, vmem_limit_bytes=VMEM_BYTES)
    vmem = pl.BlockSpec(memory_space=pltpu.VMEM)
    smem = pl.BlockSpec(memory_space=pltpu.SMEM)
    anywhere = pl.BlockSpec(memory_space=pl.ANY)
    pieces = len(halo_pieces(bricks))
    dma = pltpu.SemaphoreType.DMA
    own = (DIRS, bricks[1], rows, LANES)
    gathered = pl.pallas_call(
        functools.partial(assemble_kernel, devices, bricks),
        out_shape=jax.ShapeDtypeStruct(
            (DIRS + 1, grid[0], grid[1], devices[2], bricks[2], LANES), jnp.float32
        ),
        in_specs=[smem, vmem] + [anywhere] * 4,
        out_specs=vmem,
        scratch_shapes=[
            pltpu.VMEM((3,) + own, jnp.float32),
            pltpu.VMEM((3,) + own, jnp.float32),
            pltpu.VMEM(own, jnp.float32),
            pltpu.VMEM((3, DIRS, bricks[1], chunks, bricks[2], LANES), jnp.float32),
            pltpu.VMEM((10, len(GROUPS), LANES, LANES), jnp.float32),
            pltpu.VMEM((len(GROUPS), SUMS, 8, LANES), jnp.float32),
            dma((3, DIRS)),
            dma((pieces,)),
            dma((pieces,)),
            dma((pieces,)),
            dma((2, devices[0])),
            dma((devices[0],)),
            dma((4, devices[0])),
            dma((2, devices[0])),
            dma((devices[0],)),
            dma((devices[2] - 1, devices[0], devices[1])),
            dma((devices[2] - 1, devices[0], devices[1])),
        ],
        compiler_params=params(collective_id=0, has_side_effects=True),
        name="assemble",
    )(
        jnp.transpose(blocks, (1, 2, 3, 0)).reshape(bricks[1], bricks[2], DIRS),
        jnp.transpose(affines, (1, 2, 3, 0)).reshape(bricks[1], bricks[2], 12),
        filled(source_points),
        split(target_points),
        filled(normals),
        filled(weights),
    )
    update, residual = pl.pallas_call(
        functools.partial(solve_kernel, grid, bricks),
        out_shape=[jax.ShapeDtypeStruct(bricks[1:] + (12,), jnp.float32)] * 2,
        in_specs=[smem, vmem],
        out_specs=[vmem, vmem],
        scratch_shapes=[
            pltpu.VMEM((DIRS + 1, LANES // 4, 8, span // 2), jnp.float32),
            pltpu.VMEM((36, 8, span // 2), jnp.float32),
            pltpu.VMEM((span // 2, LANES), jnp.float32),
        ],
        compiler_params=params(),
        name="solve",
    )(anchor, gathered.reshape(DIRS + 1, span, LANES))

    def placed(value):
        return jnp.transpose(value, (2, 0, 1)).reshape((12,) + bricks)

    return placed(update), placed(residual)


def solution(mesh):
    points = P(None, None, "gx", "gy", "gz", None)
    tiles = P(None, "gx", "gy", "gz")
    return jax.shard_map(
        on_device,
        mesh=mesh,
        in_specs=(points, points, points, P(None, "gx", "gy", "gz", None), tiles, tiles, P()),
        out_specs=(tiles, tiles),
        check_vma=False,
    )
```

```python
import functools

import jax
import jax.numpy as jnp
from jax import lax
from jax.experimental import pallas as pl
from jax.experimental.pallas import tpu as pltpu
from jax.sharding import PartitionSpec as P

BLOCK = 256
ITERS = 10
SPACING = 0.5
DAMPING = 1.0
OFFSETS = (
    (1, 0, 0),
    (0, 1, 0),
    (0, 0, 1),
    (1, 1, -1),
    (1, -1, 1),
    (-1, 1, 1),
    (1, 1, 0),
    (1, 0, 1),
    (0, 1, 1),
    (1, 1, 1),
    (1, -1, 0),
    (0, 1, -1),
    (-1, 0, 1),
)
DIRS = len(OFFSETS)
LANES = 128
AXES = ("gx", "gy", "gz")
MESH = pl.DeviceIdType.MESH
VMEM_BYTES = 60 * 1024 * 1024

NORMAL_PAIRS = [(c, k) for c in range(3) for k in range(c, 3)]
POINT_PAIRS = [(e, k) for e in range(3) for k in range(e, 3)]
PAIR_ROWS = 96
THERE_ROWS = 36
SPILL = PAIR_ROWS + THERE_ROWS - LANES
SUMS = PAIR_ROWS + 2 * THERE_ROWS
SPILL_LANE = SPILL + THERE_ROWS
AFFINE_LANE = SPILL_LANE + SPILL * DIRS
SEND_ORDER = (3, 4, 5, 9, 7, 12, 0, 6, 10, 8, 11, 1, 2)
GROUPS = ((1, 2, 8, 11), (3, 4, 5, 9), (7, 12, 0, 6), (10,))
ROW_OF = {d: place for place, d in enumerate(d for group in GROUPS for d in group)}
DIRECTION_OF = {place: d for d, place in ROW_OF.items()}
CHUNKS = ((0, 4), (4, 8), (8, 12), (12, DIRS + 1))
LINE_DIRECT = (True, True, True, True)
FAR_DIRECT = (True, True, True, True)
ROUNDS_BEFORE = ((), (0,), (0, 0), (0, 0, 0))


def normal_pair(c, k):
    return NORMAL_PAIRS.index((min(c, k), max(c, k)))


def point_pair(e, k):
    return POINT_PAIRS.index((min(e, k), max(e, k)))


def moves(step, length):
    if step == 0:
        return [(slice(0, length), slice(0, length), 0)]
    if step > 0:
        return [
            (slice(step, length), slice(0, length - step), 0),
            (slice(0, step), slice(length - step, length), -1),
        ]
    return [
        (slice(0, length + step), slice(-step, length), 0),
        (slice(length + step, length), slice(0, -step), 1),
    ]


def halo_pieces(bricks):
    pieces = []
    for d in SEND_ORDER:
        dx, dy, dz = OFFSETS[d]
        for y_from, y_to, y_step in moves(dy, bricks[1]):
            for z_from, z_to, z_step in moves(dz, bricks[2]):
                pieces.append((d, (y_from, z_from), (y_to, z_to), (-dx, y_step, z_step)))
    return pieces


def all_of(conditions):
    result = None
    for condition in conditions:
        result = condition if result is None else jnp.logical_and(result, condition)
    return result


class Solver:
    def __init__(self, devices, bricks, blocks, turned):
        self.grid = tuple(devices[axis] * bricks[axis] for axis in range(3))
        self.bricks = bricks
        self.blocks = blocks
        self.turned = turned

    def load(self, parts, r):
        half = self.blocks.shape[3]
        many = LANES // 8
        d = DIRECTION_OF.get(r, DIRS)
        for start in range(0, half, LANES):
            first = parts[pl.ds(start // 8, many), r].reshape(LANES, LANES).T
            second = parts[pl.ds((half + start) // 8, many), r].reshape(LANES, LANES).T
            for i in range(LANES // 4):
                self.blocks[d, i, :, pl.ds(start, LANES)] = jnp.concatenate(
                    [first[4 * i : 4 * i + 4], second[4 * i : 4 * i + 4]], axis=0
                )

    def run(self, anchor, update_out, residual_out, tiles):
        solve(self.grid, self.bricks, anchor, update_out, residual_out, self.blocks, self.turned, tiles)


def solve(grid, bricks, anchor, update_out, residual_out, blocks, turned, tiles):
    count_x, count_y, count_z = grid
    _, side_y, side_z = bricks
    half = blocks.shape[3]
    line = count_y * side_z
    plane = count_x * line
    lane = lax.broadcasted_iota(jnp.int32, (8, half), 1)
    sub = lax.broadcasted_iota(jnp.int32, (8, half), 0)
    column = sub % 4
    low = sub < 4

    def ahead(value, offset, sign=1):
        dx, dy, dz = (sign * part for part in offset)
        shift = dx * line + dy * side_z + dz
        result = pltpu.roll(value, (-shift) % half, 1)
        if dz:
            cross = shift + dz * (plane - side_z)
            other = pltpu.roll(value, (-cross) % half, 1)
            swapped = pltpu.roll(other, 4, 0)
            if plane != half:
                stays = (lane + cross >= 0) & (lane + cross < half)
                swapped = jnp.where(stays, other, swapped)
            edge = side_z - 1 if dz > 0 else 0
            result = jnp.where(lane % side_z == edge, swapped, result)
        return result

    def spread(value, e):
        return jnp.where(low, value[e : e + 1], value[4 + e : 5 + e])

    def butterfly(first, second, span):
        takes_first = (column & span) == 0
        return jnp.where(takes_first, first, pltpu.roll(second, span, 0)) + jnp.where(
            takes_first, pltpu.roll(first, 8 - span, 0), second
        )

    def columns_summed(four):
        return butterfly(butterfly(four[0], four[1], 1), butterfly(four[2], four[3], 1), 2)

    def total(terms):
        terms = list(terms)
        while len(terms) > 1:
            terms = [
                terms[i] + terms[i + 1] if i + 1 < len(terms) else terms[i]
                for i in range(0, len(terms), 2)
            ]
        return terms[0]

    def transposed(d, spreads):
        return [
            total(
                blocks[d, normal_pair(c, k) * 4 + e] * spreads[c][e]
                for c in range(3)
                for e in range(4)
            )
            for k in range(3)
        ]

    def operate(vector, shifted=False):
        spreads = [[spread(vector[c], e) for e in range(4)] for c in range(3)]
        result = transposed(DIRS, spreads)
        sums = [[None] * 4 for _ in range(3)]
        back = [None] * 3
        for d, offset in enumerate(OFFSETS):
            near = [ahead(vector[k], offset) for k in range(3)]
            here = spreads
            if shifted:
                near = [
                    near[k] + jnp.where(column == 3, SPACING * offset[k], 0.0) for k in range(3)
                ]
                here = [
                    spreads[c][:3] + [spreads[c][3] - SPACING * offset[c]] for c in range(3)
                ]
            sent = transposed(d, here)
            for c in range(3):
                for e in range(4):
                    term = total(
                        blocks[d, normal_pair(c, k) * 4 + e] * near[k] for k in range(3)
                    )
                    sums[c][e] = term if sums[c][e] is None else sums[c][e] + term
            for k in range(3):
                term = ahead(sent[k], offset, -1)
                back[k] = term if back[k] is None else back[k] + term
        return [result[k] - back[k] - columns_summed(sums[k]) for k in range(3)]

    def rows_of(value):
        return [jnp.concatenate([value[f : f + 1], value[4 + f : 5 + f]], axis=0) for f in range(4)]

    both = []
    for g in range(THERE_ROWS // 4):
        value = blocks[DIRS, SPILL // 4 + g]
        for d, offset in enumerate(OFFSETS):
            group = PAIR_ROWS // 4 + g
            if group < LANES // 4:
                term = blocks[d, group]
            else:
                term = blocks[DIRS, SPILL_LANE // 4 + d]
            value = value + ahead(term, offset, -1)
        both.append(value)
    unit = [(column == k).astype(jnp.float32) for k in range(3)]
    affine = [blocks[DIRS, AFFINE_LANE // 4 + k] + unit[k] for k in range(3)]
    diagonal = []
    for s in range(6):
        edge = None
        for d, offset in enumerate(OFFSETS):
            term = ahead(blocks[d, s * 4 + 3], offset, -1)
            edge = term if edge is None else edge + term
        for e in range(4):
            term = total(blocks[d, s * 4 + e] for d in range(DIRS))
            edge = edge + jnp.where(column == e, spread(term, 3), 0.0)
        for e in range(3):
            value = spread(edge, e)
            for f in range(3):
                i = s * 6 + point_pair(e, f)
                value = jnp.where(column == f, spread(both[i // 4], i % 4), value)
            diagonal.append(value)
        diagonal.append(edge)
    for i, value in enumerate(diagonal):
        blocks[DIRS, i] = value

    brick_z = lane // plane + jnp.where(low, 0, half // plane)
    flat = lane % plane // side_z * count_z + brick_z * side_z + lane % side_z
    keep = (flat != anchor[0]).astype(jnp.float32)
    rhs = [-(keep * value) for value in operate(affine, True)]

    matrix = []
    for c in range(3):
        for e in range(4):
            row = []
            for k in range(3):
                value = blocks[DIRS, normal_pair(c, k) * 4 + e]
                if c == k:
                    eye = (column == e).astype(jnp.float32)
                    damped = value + DAMPING * eye
                    blocks_value = keep * damped + (1.0 - keep) * eye
                else:
                    blocks_value = keep * value
                row.append(blocks_value)
            matrix.append(row)
    for s, (c, k) in enumerate(NORMAL_PAIRS):
        if c == k:
            for e in range(4):
                value = blocks[DIRS, s * 4 + e]
                blocks[DIRS, s * 4 + e] = value + DAMPING * (column == e).astype(jnp.float32)
    for pivot in range(12):
        c, e = divmod(pivot, 4)
        here = matrix[pivot]
        factor = 1.0 / spread(here[c], e)
        at_pivot = column == e
        scaled = [here[k] * factor for k in range(3)]
        scaled[c] = jnp.where(at_pivot, factor, scaled[c])
        for a in range(12):
            if a == pivot:
                matrix[a] = scaled
            else:
                row = list(matrix[a])
                entry = spread(row[c], e)
                row[c] = jnp.where(at_pivot, 0.0, row[c])
                matrix[a] = [row[k] - entry * scaled[k] for k in range(3)]
    for a in range(12):
        for k in range(3):
            turned[a * 3 + k] = matrix[a][k]

    def precondition(vector):
        spreads = [[spread(vector[c], e) for e in range(4)] for c in range(3)]
        return [
            total(
                turned[(4 * c + e) * 3 + k] * spreads[c][e] for c in range(3) for e in range(4)
            )
            for k in range(3)
        ]

    def dot(left, right):
        return jnp.sum(total(left[k] * right[k] for k in range(3)), keepdims=True)

    first = precondition(rhs)

    def step(_, carry):
        update, residual, direction, inner_now = carry
        along = [keep * value for value in operate(direction)]
        alpha = inner_now / dot(direction, along)
        update = [update[k] + alpha * direction[k] for k in range(3)]
        residual = [residual[k] - alpha * along[k] for k in range(3)]
        scaled = precondition(residual)
        inner_next = dot(residual, scaled)
        beta = inner_next / inner_now
        direction = [scaled[k] + beta * direction[k] for k in range(3)]
        return update, residual, direction, inner_next

    start = ([jnp.zeros_like(value) for value in rhs], rhs, first, dot(rhs, first))
    update, residual, _, _ = lax.fori_loop(0, ITERS, step, start)

    at_x, at_y, at_z = (lax.axis_index(name) for name in AXES)
    bricks_half = half // plane
    upper = at_z // bricks_half
    base = (at_z - upper * bricks_half) * plane + at_x * line + at_y * side_y * side_z
    chosen = [jnp.where(upper == 0, v[:4], v[4:]) for v in update + residual]
    chosen.append(jnp.zeros((LANES - 24, half), jnp.float32))
    tall = jnp.concatenate(chosen, axis=0)
    for start in range(0, half, LANES):
        tiles[pl.ds(start, LANES), :] = tall[:, start : start + LANES].T
    rows = tiles[pl.ds(pl.multiple_of(base, 8), side_y * side_z), :]
    for y in range(side_y):
        row = rows[y * side_z : (y + 1) * side_z]
        update_out[y] = row[:, :12]
        residual_out[y] = row[:, 12:24]


def step_kernel(
    devices, bricks,
    anchor, count_in, affine_in, source, target, normal, weight,
    update_out, residual_out,
    count, affine, out, blocks, turned_inverse, tiles, small_sem,
    own_p, own_n, own_w, there, turned, acc,
    load_sem, stay_sem, halo_send, halo_recv,
    line_send, direct_send, line_recv, side_send, side_recv, core_send, core_recv,
):
    count_x, count_y, count_z = devices
    _, side_y, side_z = bricks
    at = tuple(lax.axis_index(name) for name in AXES)
    at_x, at_y, at_z = at
    pieces = halo_pieces(bricks)
    chunks = source.shape[3] // side_z

    def in_mesh(offset):
        return all_of(
            [
                (at[axis] + step >= 0) & (at[axis] + step < devices[axis])
                for axis, step in enumerate(offset)
                if step
            ]
        )

    def beside(offset):
        return tuple(
            jnp.clip(at[axis] + step, 0, devices[axis] - 1) if step else at[axis]
            for axis, step in enumerate(offset)
        )

    near_y = [at_y + 1 - 2 * (at_y % 2), (at_y + 2) % count_y]
    near_y.append((near_y[0] + 2) % count_y)

    small = (
        pltpu.make_async_copy(count_in, count, small_sem.at[0]),
        pltpu.make_async_copy(affine_in, affine, small_sem.at[1]),
    )
    for copy in small:
        copy.start()

    loads = []
    for g, group in enumerate(GROUPS):
        for d in group:
            loads.append(
                (
                    pltpu.make_async_copy(source.at[:, d], own_p.at[:, d], load_sem.at[0, d]),
                    pltpu.make_async_copy(normal.at[:, d], own_n.at[:, d], load_sem.at[1, d]),
                    pltpu.make_async_copy(weight.at[d], own_w.at[d], load_sem.at[2, d]),
                )
            )
            for copy in loads[-1]:
                copy.start()
    loads = dict(zip([d for group in GROUPS for d in group], loads))

    zeros = jnp.zeros(there.shape[2:], jnp.float32)
    for c in range(3):
        for d in range(DIRS):
            there[c, d] = zeros

    barrier = pltpu.get_barrier_semaphore()
    steps = {piece[3] for piece in pieces if any(piece[3])}
    steps |= {tuple(-s for s in step) for step in steps}
    steps |= {(k, 0, 0) for k in range(1 - count_x, count_x) if k}
    steps = sorted(steps)
    expected = 0
    for step in steps:
        there_is = in_mesh(step)

        @pl.when(there_is)
        def _(step=step):
            pl.semaphore_signal(barrier, inc=1, device_id=beside(step), device_id_type=MESH)

        expected = expected + there_is.astype(jnp.int32)
    for other in near_y:
        pl.semaphore_signal(barrier, inc=1, device_id=(at_x, other, at_z), device_id_type=MESH)
    for k in range(1, count_z):
        pl.semaphore_signal(
            barrier, inc=1, device_id=(at_x, at_y, (at_z + k) % count_z), device_id_type=MESH
        )
    pl.semaphore_wait(barrier, expected + (3 + count_z - 1))

    def spot(ref, d, where):
        return ref.at[:, d, where[0], :, where[1], :]

    def halo(i):
        d, start, end, step = pieces[i]
        return pltpu.make_async_remote_copy(
            src_ref=spot(target, d, start),
            dst_ref=spot(there, d, end),
            send_sem=halo_send.at[i],
            recv_sem=halo_recv.at[i],
            device_id=beside(step),
            device_id_type=MESH,
        )

    def stay(i):
        d, start, end, _ = pieces[i]
        return pltpu.make_async_copy(spot(target, d, start), spot(there, d, end), stay_sem.at[i])

    for i, piece in enumerate(pieces):
        if any(piece[3]):

            @pl.when(in_mesh(piece[3]))
            def _(i=i):
                halo(i).start()

        else:
            stay(i).start()

    inside = {}
    for axis in range(3):
        length = devices[axis] * bricks[axis]
        for place in range(bricks[axis]):
            for step in (-1, 1):
                ahead = at[axis] * bricks[axis] + place + step
                inside[axis, place, step] = ((ahead >= 0) & (ahead < length)).astype(jnp.int32)

    for copy in small:
        copy.wait()
    rows = chunks * side_z
    sub = lax.broadcasted_iota(jnp.int32, (rows, LANES), 0)
    lane = lax.broadcasted_iota(jnp.int32, (rows, LANES), 1)
    point = lane + LANES * (sub // side_z)

    def live_weight(d, y):
        limit = None
        for z in range(side_z):
            value = count[y, z, d] * BLOCK
            for axis, place in enumerate((0, y, z)):
                if OFFSETS[d][axis]:
                    value = value * inside[axis, place, OFFSETS[d][axis]]
            limit = value if limit is None else jnp.where(sub % side_z == z, value, limit)
        return jnp.where(point < limit, own_w[d, y], 0.0)

    def turn(parts):
        missing = LANES - rows * len(parts)
        if missing:
            parts = parts + [jnp.zeros((missing, LANES), jnp.float32)]
        return jnp.concatenate(parts, axis=0).T

    step = 32

    def summed(g, kinds):
        def body(chunk, carry):
            spots = pl.ds(pl.multiple_of(chunk * step, step), step)
            p = [turned[c, g, spots, :] for c in range(3)] + [None]
            q = [turned[7 + c, g, spots, :] for c in range(3)] + [None] if kinds == "there" else None
            n = [turned[3 + c, g, spots, :] for c in range(3)]
            w = turned[6, g, spots, :]

            def times(left, right):
                if left is None:
                    return right
                return left if right is None else left * right

            def add(row, value):
                acc[g, row] += jnp.sum(value.reshape(step // 8, 8, LANES), axis=0)

            wn = [w * n[c] for c in range(3)]
            weighted = [wn[c] * n[k] for c, k in NORMAL_PAIRS]
            if kinds == "here":
                for e in range(4):
                    for s in range(6):
                        add(s * 16 + e * 4 + 3, times(weighted[s], p[e]))
                for place, (e, k) in enumerate(POINT_PAIRS):
                    product = p[e] * p[k]
                    for s in range(6):
                        add(PAIR_ROWS + THERE_ROWS + s * 6 + place, weighted[s] * product)
            else:
                for e in range(4):
                    for k in range(3):
                        product = times(p[e], q[k])
                        for s in range(6):
                            add(s * 16 + e * 4 + k, weighted[s] * product)
                for place, (e, k) in enumerate(POINT_PAIRS):
                    product = q[e] * q[k]
                    for s in range(6):
                        add(PAIR_ROWS + s * 6 + place, weighted[s] * product)
            return carry

        lax.fori_loop(0, LANES // step, body, 0)

    acc[...] = jnp.zeros_like(acc)

    def here(g):
        group = GROUPS[g]
        for d in group:
            for copy in loads[d]:
                copy.wait()
        for c in range(3):
            turned[c, g] = turn([own_p[c, d, y] for d in group for y in range(side_y)])
            turned[3 + c, g] = turn([own_n[c, d, y] for d in group for y in range(side_y)])
        turned[6, g] = turn([live_weight(d, y) for d in group for y in range(side_y)])
        summed(g, "here")

    there_rows = there.reshape(3, DIRS, side_y, rows, LANES)
    last = [None] * side_y
    mine = out.at[at_z, at_x, at_y]

    def tiles_of(values):
        result = values[0]
        for y in range(1, side_y):
            result = jnp.where(sub // side_z == y, values[y], result)
        return result

    def there_sums(g):
        group = GROUPS[g]
        for i, piece in enumerate(pieces):
            if piece[0] in group:
                if any(piece[3]):

                    @pl.when(in_mesh(tuple(-s for s in piece[3])))
                    def _(i=i):
                        halo(i).wait_recv()

                else:
                    stay(i).wait()
        for c in range(3):
            turned[7 + c, g] = turn([there_rows[c, d, y] for d in group for y in range(side_y)])
        summed(g, "there")
        whole = [jnp.sum(acc[g, r : r + 8], axis=1) for r in range(0, SUMS, 8)]
        main = jnp.concatenate(whole[: LANES // 8], axis=0).T
        rest = whole[LANES // 8 :] + [jnp.zeros((2 * LANES - SUMS, LANES), jnp.float32)]
        rest = jnp.concatenate(rest, axis=0).T

        def all_chunks(value):
            span = rows // 2
            while span >= side_z:
                value = value + pltpu.roll(value, span, 0)
                span //= 2
            return value

        for place, d in enumerate(group):
            main_rows = []
            for y in range(side_y):
                first = (place * side_y + y) * rows
                main_rows.append(all_chunks(main[first : first + rows]))
                value = all_chunks(rest[first : first + rows])
                spill = pltpu.roll(jnp.where(lane < SPILL, value, 0.0), SPILL_LANE + SPILL * d, 1)
                value = jnp.where(lane < SPILL, 0.0, value) + spill
                last[y] = value if last[y] is None else last[y] + value
            mine[ROW_OF[d]] = tiles_of(main_rows)
        if g < len(GROUPS) - 1:
            return
        pad = [jnp.zeros((rows, AFFINE_LANE), jnp.float32)]
        pad.append(jnp.concatenate([affine[y] for y in range(side_y)], axis=0))
        pad.append(jnp.zeros((rows, LANES - AFFINE_LANE - affine.shape[2]), jnp.float32))
        mine[DIRS] = tiles_of(last) + jnp.concatenate(pad, axis=1)

    def send(c, x, y, z, send_sem, recv_sem, other):
        first, end = CHUNKS[c]
        part = out.at[z, x, y, pl.ds(first, end - first)]
        return pltpu.make_async_remote_copy(
            src_ref=part,
            dst_ref=part,
            send_sem=send_sem,
            recv_sem=recv_sem,
            device_id=other,
            device_id_type=MESH,
        )

    def along(c, x, sign):
        other = (jnp.clip(at_x + sign, 0, count_x - 1), at_y, at_z)
        way = (sign + 1) // 2
        return send(c, x, at_y, at_z, line_send.at[c, way, x], line_recv.at[c, x], other)

    def direct(c, step):
        other = (jnp.clip(at_x + step, 0, count_x - 1), at_y, at_z)
        sem = direct_send.at[c, step + count_x - 1]
        return send(c, at_x, at_y, at_z, sem, line_recv.at[c, at_x], other)

    def across(c, x, way):
        other = (at_x, near_y[way], at_z)
        return send(c, x, at_y, at_z, side_send.at[c, way, x], side_recv.at[c, way, x], other)

    def across_in(c, x, way):
        other = (at_x, near_y[way], at_z)
        sems = side_send.at[c, way, x], side_recv.at[c, way, x]
        return send(c, x, near_y[way], at_z, *sems, other)

    def far_out(c, x, way):
        other = (at_x, near_y[1 - way], at_z)
        sems = side_send.at[c, 2, x], side_recv.at[c, 2, x]
        return send(c, x, near_y[way], at_z, *sems, other)

    def core_out(c, x, y, k):
        other = (at_x, at_y, (at_z + k) % count_z)
        sems = core_send.at[c, k - 1, x, y], core_recv.at[c, k - 1, x, y]
        return send(c, x, y, at_z, *sems, other)

    def core_in(c, x, y, k):
        from_z = (at_z + count_z - k) % count_z
        sems = core_send.at[c, k - 1, x, y], core_recv.at[c, k - 1, x, y]
        return send(c, x, y, from_z, *sems, (at_x, at_y, from_z))

    def to_cores(c, x, y):
        for k in range(1, count_z):
            core_out(c, x, y, k).start()

    def spread(c, x):
        for way in range(3 if FAR_DIRECT[c] else 2):
            across(c, x, way).start()
        to_cores(c, x, at_y)

    def own_out(c):
        for step in [k for far in range(count_x - 1, 0, -1) for k in (far, -far)]:
            if LINE_DIRECT[c] or abs(step) == 1:

                @pl.when((at_x + step >= 0) & (at_x + step < count_x))
                def _(step=step):
                    if LINE_DIRECT[c]:
                        direct(c, step).start()
                    else:
                        along(c, at_x, step).start()

        spread(c, at_x)

    def line_arrived(c, x, sign):
        along(c, x, sign).wait_recv()
        if not LINE_DIRECT[c]:

            @pl.when((at_x + sign >= 0) & (at_x + sign < count_x))
            def _():
                along(c, x, sign).start()

        spread(c, x)

    def side_arrived(c, x, sign):
        for way in range(2):
            across_in(c, x, way).wait_recv()
            if not FAR_DIRECT[c]:

                @pl.when(x % 2 == way)
                def _(way=way):
                    far_out(c, x, way).start()

            to_cores(c, x, near_y[way])

    def far_arrived(c, x, sign):
        across_in(c, x, 2).wait_recv()
        to_cores(c, x, near_y[2])

    def both_ways(c, distance, body):
        if distance == 0:
            body(c, at_x, 0)
        elif 0 < distance < count_x:

            @pl.when(at_x - distance >= 0)
            def _():
                body(c, at_x - distance, 1)

            @pl.when(at_x + distance < count_x)
            def _():
                body(c, at_x + distance, -1)

    def gather_round(c, r):
        if r == 0:
            own_out(c)
            return
        both_ways(c, r, line_arrived)
        both_ways(c, r - 1, side_arrived)
        both_ways(c, r - 2, far_arrived)

    rounds = count_x + 2
    done = [0] * len(GROUPS)

    def advance(c, many):
        for _ in range(many):
            if done[c] < rounds:
                gather_round(c, done[c])
                done[c] += 1

    for g in range(len(GROUPS)):
        here(g)
    for g in range(len(GROUPS)):
        for c, many in enumerate(ROUNDS_BEFORE[g]):
            advance(c, many)
        there_sums(g)
        advance(g, 1)
    while min(done) < rounds:
        for c in range(len(GROUPS)):
            if done[c] < rounds:
                advance(c, 1)

    solver = Solver(devices, bricks, blocks, turned_inverse)
    parts = out.reshape(out.shape[0] * count_x * count_y, DIRS + 1, 8, LANES)
    for c, (first, end) in enumerate(CHUNKS):

        def cores(i, carry, c=c):
            for k in range(1, count_z):
                core_in(c, i // count_y, i % count_y, k).wait_recv()
            return carry

        lax.fori_loop(0, count_x * count_y, cores, 0)
        for r in range(first, end):
            solver.load(parts, r)

    def sent(x, carry):
        for c in range(len(GROUPS)):
            for sign in (1, -1):
                if not LINE_DIRECT[c]:
                    passed = (at_x + sign >= 0) & (at_x + sign < count_x)
                    passed = passed & ((x <= at_x) if sign > 0 else (x >= at_x))

                    @pl.when(passed)
                    def _(sign=sign, c=c):
                        along(c, x, sign).wait_send()

            for way in range(3 if FAR_DIRECT[c] else 2):
                across(c, x, way).wait_send()
                if not FAR_DIRECT[c]:

                    @pl.when(x % 2 == way)
                    def _(way=way, c=c):
                        far_out(c, x, way).wait_send()

            def cores(y, inner, c=c):
                for k in range(1, count_z):
                    core_out(c, x, y, k).wait_send()
                return inner

            lax.fori_loop(0, count_y, cores, 0)
        return carry

    lax.fori_loop(0, count_x, sent, 0)
    for c in range(len(GROUPS)):
        for step in range(1 - count_x, count_x):
            if step and LINE_DIRECT[c]:

                @pl.when((at_x + step >= 0) & (at_x + step < count_x))
                def _(c=c, step=step):
                    direct(c, step).wait_send()

    for i, piece in enumerate(pieces):
        if any(piece[3]):

            @pl.when(in_mesh(piece[3]))
            def _(i=i):
                halo(i).wait_send()

    solver.run(anchor, update_out, residual_out, tiles)


def on_device(source_points, target_points, normals, weights, blocks, affines, anchor):
    bricks = source_points.shape[2:5]
    points = source_points.shape[5]
    devices = tuple(lax.axis_size(name) for name in AXES)
    grid = tuple(devices[axis] * bricks[axis] for axis in range(3))
    span = grid[0] * grid[1] * grid[2]
    chunks = points // LANES
    rows = chunks * bricks[2]
    assert bricks[0] == 1 and rows == 8 and devices[2] % 2 == 0 and devices[1] == 4
    assert bricks[1] * bricks[2] == 8
    assert span % (2 * LANES) == 0 and len(GROUPS[0]) * bricks[1] * rows == LANES

    def split(value):
        lead = value.shape[:-5]
        value = value.reshape(lead + (DIRS, bricks[1], bricks[2], chunks, LANES))
        return jnp.swapaxes(value, -3, -2)

    def filled(value):
        value = split(value)
        return value.reshape(value.shape[:-3] + (rows, LANES))

    params = functools.partial(pltpu.CompilerParams, vmem_limit_bytes=VMEM_BYTES)
    vmem = pl.BlockSpec(memory_space=pltpu.VMEM)
    smem = pl.BlockSpec(memory_space=pltpu.SMEM)
    anywhere = pl.BlockSpec(memory_space=pl.ANY)
    pieces = len(halo_pieces(bricks))
    dma = pltpu.SemaphoreType.DMA
    groups = len(GROUPS)
    own = (DIRS, bricks[1], rows, LANES)
    update, residual = pl.pallas_call(
        functools.partial(step_kernel, devices, bricks),
        out_shape=[jax.ShapeDtypeStruct(bricks[1:] + (12,), jnp.float32)] * 2,
        in_specs=[smem] + [anywhere] * 6,
        out_specs=[vmem, vmem],
        scratch_shapes=[
            pltpu.SMEM(bricks[1:] + (DIRS,), jnp.int32),
            pltpu.VMEM(bricks[1:] + (12,), jnp.float32),
            pltpu.VMEM(
                (devices[2], devices[0], devices[1], DIRS + 1, 8, LANES), jnp.float32
            ),
            pltpu.VMEM((DIRS + 1, LANES // 4, 8, span // 2), jnp.float32),
            pltpu.VMEM((36, 8, span // 2), jnp.float32),
            pltpu.VMEM((span // 2, LANES), jnp.float32),
            dma((2,)),
            pltpu.VMEM((3,) + own, jnp.float32),
            pltpu.VMEM((3,) + own, jnp.float32),
            pltpu.VMEM(own, jnp.float32),
            pltpu.VMEM((3, DIRS, bricks[1], chunks, bricks[2], LANES), jnp.float32),
            pltpu.VMEM((10, len(GROUPS), LANES, LANES), jnp.float32),
            pltpu.VMEM((len(GROUPS), SUMS, 8, LANES), jnp.float32),
            dma((3, DIRS)),
            dma((pieces,)),
            dma((pieces,)),
            dma((pieces,)),
            dma((groups, 2, devices[0])),
            dma((groups, 2 * devices[0] - 1)),
            dma((groups, devices[0])),
            dma((groups, 3, devices[0])),
            dma((groups, 3, devices[0])),
            dma((groups, devices[2] - 1, devices[0], devices[1])),
            dma((groups, devices[2] - 1, devices[0], devices[1])),
        ],
        compiler_params=params(collective_id=0, has_side_effects=True),
        name="step",
    )(
        anchor,
        jnp.transpose(blocks, (1, 2, 3, 0)).reshape(bricks[1], bricks[2], DIRS),
        jnp.transpose(affines, (1, 2, 3, 0)).reshape(bricks[1], bricks[2], 12),
        filled(source_points),
        split(target_points),
        filled(normals),
        filled(weights),
    )
    def placed(value):
        return jnp.transpose(value, (2, 0, 1)).reshape((12,) + bricks)

    return placed(update), placed(residual)


def solution(mesh):
    points = P(None, None, "gx", "gy", "gz", None)
    tiles = P(None, "gx", "gy", "gz")
    return jax.shard_map(
        on_device,
        mesh=mesh,
        in_specs=(points, points, points, P(None, "gx", "gy", "gz", None), tiles, tiles, P()),
        out_specs=(tiles, tiles),
        check_vma=False,
    )
```

```python
import functools

import jax
import jax.numpy as jnp
from jax import lax
from jax.experimental import pallas as pl
from jax.experimental.pallas import tpu as pltpu
from jax.sharding import PartitionSpec as P

BLOCK = 256
ITERS = 10
SPACING = 0.5
DAMPING = 1.0
OFFSETS = (
    (1, 0, 0),
    (0, 1, 0),
    (0, 0, 1),
    (1, 1, -1),
    (1, -1, 1),
    (-1, 1, 1),
    (1, 1, 0),
    (1, 0, 1),
    (0, 1, 1),
    (1, 1, 1),
    (1, -1, 0),
    (0, 1, -1),
    (-1, 0, 1),
)
DIRS = len(OFFSETS)
LANES = 128
AXES = ("gx", "gy", "gz")
MESH = pl.DeviceIdType.MESH
VMEM_BYTES = 60 * 1024 * 1024

NORMAL_PAIRS = [(c, k) for c in range(3) for k in range(c, 3)]
POINT_PAIRS = [(e, k) for e in range(3) for k in range(e, 3)]
PAIR_ROWS = 96
THERE_ROWS = 36
SPILL = PAIR_ROWS + THERE_ROWS - LANES
SUMS = PAIR_ROWS + 2 * THERE_ROWS
SPILL_LANE = SPILL + THERE_ROWS
AFFINE_LANE = SPILL_LANE + SPILL * DIRS
SEND_ORDER = (1, 2, 8, 11, 3, 4, 9, 5, 7, 0, 6, 12, 10)
GROUPS = ((1, 2, 8, 11), (3, 4, 5, 9), (7, 12, 0, 6), (10,))
ROW_OF = {d: place for place, d in enumerate(d for group in GROUPS for d in group)}
DIRECTION_OF = {place: d for d, place in ROW_OF.items()}
CHUNKS = ((0, 4), (4, 8), (8, 12), (12, DIRS + 1))
DIRECT = (0, 1, 2, 3)
SCHEDULE = (
    "here 0", "here 1", "here 2", "here 3", "there 0", "line 0", "there 1", "line 1",
    "there 2", "line 2", "side 0", "there 3", "line 3", "side 1", "side 2", "far 0", "side 3",
    "far 1", "core 0", "far 2", "core 1", "load 0", "far 3", "core 2", "load 1", "core 3",
    "load 2", "load 3",
)


def normal_pair(c, k):
    return NORMAL_PAIRS.index((min(c, k), max(c, k)))


def point_pair(e, k):
    return POINT_PAIRS.index((min(e, k), max(e, k)))


def moves(step, length):
    if step == 0:
        return [(slice(0, length), slice(0, length), 0)]
    if step > 0:
        return [
            (slice(step, length), slice(0, length - step), 0),
            (slice(0, step), slice(length - step, length), -1),
        ]
    return [
        (slice(0, length + step), slice(-step, length), 0),
        (slice(length + step, length), slice(0, -step), 1),
    ]


def halo_pieces(bricks):
    pieces = []
    for d in SEND_ORDER:
        dx, dy, dz = OFFSETS[d]
        for y_from, y_to, y_step in moves(dy, bricks[1]):
            for z_from, z_to, z_step in moves(dz, bricks[2]):
                pieces.append((d, (y_from, z_from), (y_to, z_to), (-dx, y_step, z_step)))
    return pieces


def all_of(conditions):
    result = None
    for condition in conditions:
        result = condition if result is None else jnp.logical_and(result, condition)
    return result


class Solver:
    def __init__(self, devices, bricks, blocks, turned):
        self.grid = tuple(devices[axis] * bricks[axis] for axis in range(3))
        self.bricks = bricks
        self.blocks = blocks
        self.turned = turned

    def load(self, parts, r):
        half = self.blocks.shape[3]
        many = LANES // 8
        d = DIRECTION_OF.get(r, DIRS)
        for start in range(0, half, LANES):
            first = parts[pl.ds(start // 8, many), r].reshape(LANES, LANES).T
            second = parts[pl.ds((half + start) // 8, many), r].reshape(LANES, LANES).T
            for i in range(LANES // 4):
                self.blocks[d, i, :, pl.ds(start, LANES)] = jnp.concatenate(
                    [first[4 * i : 4 * i + 4], second[4 * i : 4 * i + 4]], axis=0
                )

    def run(self, anchor, result_out, tiles):
        solve(self.grid, self.bricks, anchor, result_out, self.blocks, self.turned, tiles)


def solve(grid, bricks, anchor, result_out, blocks, turned, tiles):
    count_x, count_y, count_z = grid
    _, side_y, side_z = bricks
    half = blocks.shape[3]
    line = count_y * side_z
    plane = count_x * line
    lane = lax.broadcasted_iota(jnp.int32, (8, half), 1)
    sub = lax.broadcasted_iota(jnp.int32, (8, half), 0)
    column = sub % 4
    low = sub < 4

    def ahead(value, offset, sign=1):
        dx, dy, dz = (sign * part for part in offset)
        shift = dx * line + dy * side_z + dz
        result = pltpu.roll(value, (-shift) % half, 1)
        if dz:
            cross = shift + dz * (plane - side_z)
            other = pltpu.roll(value, (-cross) % half, 1)
            swapped = pltpu.roll(other, 4, 0)
            if plane != half:
                stays = (lane + cross >= 0) & (lane + cross < half)
                swapped = jnp.where(stays, other, swapped)
            edge = side_z - 1 if dz > 0 else 0
            result = jnp.where(lane % side_z == edge, swapped, result)
        return result

    def spread(value, e):
        return jnp.where(low, value[e : e + 1], value[4 + e : 5 + e])

    def butterfly(first, second, span):
        takes_first = (column & span) == 0
        return jnp.where(takes_first, first, pltpu.roll(second, span, 0)) + jnp.where(
            takes_first, pltpu.roll(first, 8 - span, 0), second
        )

    def columns_summed(four):
        return butterfly(butterfly(four[0], four[1], 1), butterfly(four[2], four[3], 1), 2)

    def total(terms):
        terms = list(terms)
        while len(terms) > 1:
            terms = [
                terms[i] + terms[i + 1] if i + 1 < len(terms) else terms[i]
                for i in range(0, len(terms), 2)
            ]
        return terms[0]

    def transposed(d, spreads):
        return [
            total(
                blocks[d, normal_pair(c, k) * 4 + e] * spreads[c][e]
                for c in range(3)
                for e in range(4)
            )
            for k in range(3)
        ]

    def operate(vector, shifted=False):
        spreads = [[spread(vector[c], e) for e in range(4)] for c in range(3)]
        result = transposed(DIRS, spreads)
        sums = [[None] * 4 for _ in range(3)]
        back = [None] * 3
        for d, offset in enumerate(OFFSETS):
            near = [ahead(vector[k], offset) for k in range(3)]
            here = spreads
            if shifted:
                near = [
                    near[k] + jnp.where(column == 3, SPACING * offset[k], 0.0) for k in range(3)
                ]
                here = [
                    spreads[c][:3] + [spreads[c][3] - SPACING * offset[c]] for c in range(3)
                ]
            sent = transposed(d, here)
            for c in range(3):
                for e in range(4):
                    term = total(
                        blocks[d, normal_pair(c, k) * 4 + e] * near[k] for k in range(3)
                    )
                    sums[c][e] = term if sums[c][e] is None else sums[c][e] + term
            for k in range(3):
                term = ahead(sent[k], offset, -1)
                back[k] = term if back[k] is None else back[k] + term
        return [result[k] - back[k] - columns_summed(sums[k]) for k in range(3)]

    def rows_of(value):
        return [jnp.concatenate([value[f : f + 1], value[4 + f : 5 + f]], axis=0) for f in range(4)]

    both = []
    for g in range(THERE_ROWS // 4):
        value = blocks[DIRS, SPILL // 4 + g]
        for d, offset in enumerate(OFFSETS):
            group = PAIR_ROWS // 4 + g
            if group < LANES // 4:
                term = blocks[d, group]
            else:
                term = blocks[DIRS, SPILL_LANE // 4 + d]
            value = value + ahead(term, offset, -1)
        both.append(value)
    unit = [(column == k).astype(jnp.float32) for k in range(3)]
    affine = [blocks[DIRS, AFFINE_LANE // 4 + k] + unit[k] for k in range(3)]
    diagonal = []
    for s in range(6):
        edge = None
        for d, offset in enumerate(OFFSETS):
            term = ahead(blocks[d, s * 4 + 3], offset, -1)
            edge = term if edge is None else edge + term
        for e in range(4):
            term = total(blocks[d, s * 4 + e] for d in range(DIRS))
            edge = edge + jnp.where(column == e, spread(term, 3), 0.0)
        for e in range(3):
            value = spread(edge, e)
            for f in range(3):
                i = s * 6 + point_pair(e, f)
                value = jnp.where(column == f, spread(both[i // 4], i % 4), value)
            diagonal.append(value)
        diagonal.append(edge)
    for i, value in enumerate(diagonal):
        blocks[DIRS, i] = value

    brick_z = lane // plane + jnp.where(low, 0, half // plane)
    flat = lane % plane // side_z * count_z + brick_z * side_z + lane % side_z
    keep = (flat != anchor[0]).astype(jnp.float32)
    rhs = [-(keep * value) for value in operate(affine, True)]

    matrix = []
    for c in range(3):
        for e in range(4):
            row = []
            for k in range(3):
                value = blocks[DIRS, normal_pair(c, k) * 4 + e]
                if c == k:
                    eye = (column == e).astype(jnp.float32)
                    damped = value + DAMPING * eye
                    blocks_value = keep * damped + (1.0 - keep) * eye
                else:
                    blocks_value = keep * value
                row.append(blocks_value)
            matrix.append(row)
    for s, (c, k) in enumerate(NORMAL_PAIRS):
        if c == k:
            for e in range(4):
                value = blocks[DIRS, s * 4 + e]
                blocks[DIRS, s * 4 + e] = value + DAMPING * (column == e).astype(jnp.float32)
    for pivot in range(12):
        c, e = divmod(pivot, 4)
        here = matrix[pivot]
        factor = 1.0 / spread(here[c], e)
        at_pivot = column == e
        scaled = [here[k] * factor for k in range(3)]
        scaled[c] = jnp.where(at_pivot, factor, scaled[c])
        for a in range(12):
            if a == pivot:
                matrix[a] = scaled
            else:
                row = list(matrix[a])
                entry = spread(row[c], e)
                row[c] = jnp.where(at_pivot, 0.0, row[c])
                matrix[a] = [row[k] - entry * scaled[k] for k in range(3)]
    for a in range(12):
        for k in range(3):
            turned[a * 3 + k] = matrix[a][k]

    def precondition(vector):
        spreads = [[spread(vector[c], e) for e in range(4)] for c in range(3)]
        return [
            total(
                turned[(4 * c + e) * 3 + k] * spreads[c][e] for c in range(3) for e in range(4)
            )
            for k in range(3)
        ]

    def dot(left, right):
        value = total(left[k] * right[k] for k in range(3))
        value = total(value[:, start : start + LANES] for start in range(0, half, LANES))
        for span in (4, 2, 1):
            value = value + pltpu.roll(value, span, 0)
        return jnp.sum(value, axis=1, keepdims=True)

    first = precondition(rhs)

    def step(_, carry):
        update, residual, direction, inner_now = carry
        along = [keep * value for value in operate(direction)]
        alpha = inner_now / dot(direction, along)
        update = [update[k] + alpha * direction[k] for k in range(3)]
        residual = [residual[k] - alpha * along[k] for k in range(3)]
        scaled = precondition(residual)
        inner_next = dot(residual, scaled)
        beta = inner_next / inner_now
        direction = [scaled[k] + beta * direction[k] for k in range(3)]
        return update, residual, direction, inner_next

    start = ([jnp.zeros_like(value) for value in rhs], rhs, first, dot(rhs, first))
    update, residual, _, _ = lax.fori_loop(0, ITERS, step, start)

    at_x, at_y, at_z = (lax.axis_index(name) for name in AXES)
    bricks_half = half // plane
    upper = at_z // bricks_half
    base = (at_z - upper * bricks_half) * plane + at_x * line + at_y * side_y * side_z
    chosen = [jnp.where(upper == 0, v[:4], v[4:]) for v in update + residual]
    chosen.append(jnp.zeros((LANES - 24, half), jnp.float32))
    tall = jnp.concatenate(chosen, axis=0)
    for start in range(0, half, LANES):
        tiles[pl.ds(start, LANES), :] = tall[:, start : start + LANES].T
    rows = tiles[pl.ds(pl.multiple_of(base, 8), side_y * side_z), :]
    for y in range(side_y):
        row = rows[y * side_z : (y + 1) * side_z]
        result_out[y] = row[:, :24]


def step_kernel(
    devices, bricks,
    anchor_in, count_in, affine_in, source, target, normal, weight,
    result_out,
    anchor, count, affine, out, blocks, turned_inverse, tiles, small_sem,
    own_p, own_n, own_w, there, turned, acc,
    load_sem, stay_sem, halo_send, halo_recv,
    line_send, line_recv, side_send, side_recv, core_send, core_recv,
):
    count_x, count_y, count_z = devices
    _, side_y, side_z = bricks
    at = tuple(lax.axis_index(name) for name in AXES)
    at_x, at_y, at_z = at
    pieces = halo_pieces(bricks)
    leaving = [i for i, piece in enumerate(pieces) if any(piece[3])]
    staying = [i for i, piece in enumerate(pieces) if not any(piece[3])]
    chunks = source.shape[3] // side_z

    def in_mesh(offset):
        return all_of(
            [
                (at[axis] + step >= 0) & (at[axis] + step < devices[axis])
                for axis, step in enumerate(offset)
                if step
            ]
        )

    def beside(offset):
        return tuple(
            jnp.clip(at[axis] + step, 0, devices[axis] - 1) if step else at[axis]
            for axis, step in enumerate(offset)
        )

    near_y = [at_y + 1 - 2 * (at_y % 2), (at_y + 2) % count_y]
    near_y.append((near_y[0] + 2) % count_y)

    small = (
        pltpu.make_async_copy(count_in, count, small_sem.at[0]),
        pltpu.make_async_copy(affine_in, affine, small_sem.at[1]),
        pltpu.make_async_copy(anchor_in, anchor, small_sem.at[2]),
    )
    for copy in small:
        copy.start()

    loads = (
        pltpu.make_async_copy(source, own_p, load_sem.at[0]),
        pltpu.make_async_copy(normal, own_n, load_sem.at[1]),
        pltpu.make_async_copy(weight, own_w, load_sem.at[2]),
    )
    for copy in loads:
        copy.start()

    zeros = jnp.zeros(there.shape[2:], jnp.float32)
    for c in range(3):
        for d in range(DIRS):
            there[c, d] = zeros

    barrier = pltpu.get_barrier_semaphore()
    steps = {piece[3] for piece in pieces if any(piece[3])}
    steps |= {tuple(-s for s in step) for step in steps}
    steps |= {(k, 0, 0) for k in range(1 - count_x, count_x) if k}
    steps = sorted(steps)
    expected = 0
    for step in steps:
        there_is = in_mesh(step)

        @pl.when(there_is)
        def _(step=step):
            pl.semaphore_signal(barrier, inc=1, device_id=beside(step), device_id_type=MESH)

        expected = expected + there_is.astype(jnp.int32)
    for other in near_y:
        pl.semaphore_signal(barrier, inc=1, device_id=(at_x, other, at_z), device_id_type=MESH)
    for k in range(1, count_z):
        pl.semaphore_signal(
            barrier, inc=1, device_id=(at_x, at_y, (at_z + k) % count_z), device_id_type=MESH
        )
    pl.semaphore_wait(barrier, expected + (3 + count_z - 1))

    def spot(ref, d, where):
        return ref.at[:, d, where[0], :, where[1], :]

    def halo(i):
        d, start, end, step = pieces[i]
        return pltpu.make_async_remote_copy(
            src_ref=spot(target, d, start),
            dst_ref=spot(there, d, end),
            send_sem=halo_send.at[leaving.index(i)],
            recv_sem=halo_recv.at[leaving.index(i)],
            device_id=beside(step),
            device_id_type=MESH,
        )

    def stay(i):
        d, start, end, _ = pieces[i]
        return pltpu.make_async_copy(spot(target, d, start), spot(there, d, end), stay_sem.at[staying.index(i)])

    for i, piece in enumerate(pieces):
        if any(piece[3]):

            @pl.when(in_mesh(piece[3]))
            def _(i=i):
                halo(i).start()

        else:
            stay(i).start()

    inside = {}
    for axis in range(3):
        length = devices[axis] * bricks[axis]
        for place in range(bricks[axis]):
            for step in (-1, 1):
                ahead = at[axis] * bricks[axis] + place + step
                inside[axis, place, step] = ((ahead >= 0) & (ahead < length)).astype(jnp.int32)

    for copy in small:
        copy.wait()
    rows = chunks * side_z
    sub = lax.broadcasted_iota(jnp.int32, (rows, LANES), 0)
    lane = lax.broadcasted_iota(jnp.int32, (rows, LANES), 1)
    point = lane + LANES * (sub // side_z)

    def live_weight(d, y):
        limit = None
        for z in range(side_z):
            value = count[y, z, d] * BLOCK
            for axis, place in enumerate((0, y, z)):
                if OFFSETS[d][axis]:
                    value = value * inside[axis, place, OFFSETS[d][axis]]
            limit = value if limit is None else jnp.where(sub % side_z == z, value, limit)
        return jnp.where(point < limit, own_w[d, y], 0.0)

    def turn(parts):
        missing = LANES - rows * len(parts)
        if missing:
            parts = parts + [jnp.zeros((missing, LANES), jnp.float32)]
        return jnp.concatenate(parts, axis=0).T

    step = 32

    def summed(g, kinds):
        def body(chunk, carry):
            spots = pl.ds(pl.multiple_of(chunk * step, step), step)
            p = [turned[c, g, spots, :] for c in range(3)] + [None]
            q = [turned[7 + c, g, spots, :] for c in range(3)] + [None] if kinds == "there" else None
            n = [turned[3 + c, g, spots, :] for c in range(3)]
            w = turned[6, g, spots, :]

            def times(left, right):
                if left is None:
                    return right
                return left if right is None else left * right

            def add(row, value):
                acc[g, row] += jnp.sum(value.reshape(step // 8, 8, LANES), axis=0)

            wn = [w * n[c] for c in range(3)]
            weighted = [wn[c] * n[k] for c, k in NORMAL_PAIRS]
            if kinds == "here":
                for e in range(4):
                    for s in range(6):
                        add(s * 16 + e * 4 + 3, times(weighted[s], p[e]))
                for place, (e, k) in enumerate(POINT_PAIRS):
                    product = p[e] * p[k]
                    for s in range(6):
                        add(PAIR_ROWS + THERE_ROWS + s * 6 + place, weighted[s] * product)
            else:
                for e in range(4):
                    for k in range(3):
                        product = times(p[e], q[k])
                        for s in range(6):
                            add(s * 16 + e * 4 + k, weighted[s] * product)
                for place, (e, k) in enumerate(POINT_PAIRS):
                    product = q[e] * q[k]
                    for s in range(6):
                        add(PAIR_ROWS + s * 6 + place, weighted[s] * product)
            return carry

        lax.fori_loop(0, LANES // step, body, 0)

    acc[...] = jnp.zeros_like(acc)

    def here(g):
        group = GROUPS[g]
        if g == 0:
            for copy in loads:
                copy.wait()
        for c in range(3):
            turned[c, g] = turn([own_p[c, d, y] for d in group for y in range(side_y)])
            turned[3 + c, g] = turn([own_n[c, d, y] for d in group for y in range(side_y)])
        turned[6, g] = turn([live_weight(d, y) for d in group for y in range(side_y)])
        summed(g, "here")

    there_rows = there.reshape(3, DIRS, side_y, rows, LANES)
    last = [None] * side_y
    mine = out.at[at_z, at_x, at_y]

    def tiles_of(values):
        result = values[0]
        for y in range(1, side_y):
            result = jnp.where(sub // side_z == y, values[y], result)
        return result

    def there_sums(g):
        group = GROUPS[g]
        for i, piece in enumerate(pieces):
            if piece[0] in group:
                if any(piece[3]):

                    @pl.when(in_mesh(tuple(-s for s in piece[3])))
                    def _(i=i):
                        halo(i).wait_recv()

                else:
                    stay(i).wait()
        for c in range(3):
            turned[7 + c, g] = turn([there_rows[c, d, y] for d in group for y in range(side_y)])
        summed(g, "there")
        whole = [jnp.sum(acc[g, r : r + 8], axis=1) for r in range(0, SUMS, 8)]
        main = jnp.concatenate(whole[: LANES // 8], axis=0).T
        rest = whole[LANES // 8 :] + [jnp.zeros((2 * LANES - SUMS, LANES), jnp.float32)]
        rest = jnp.concatenate(rest, axis=0).T

        def all_chunks(value):
            span = rows // 2
            while span >= side_z:
                value = value + pltpu.roll(value, span, 0)
                span //= 2
            return value

        for place, d in enumerate(group):
            main_rows = []
            for y in range(side_y):
                first = (place * side_y + y) * rows
                main_rows.append(all_chunks(main[first : first + rows]))
                value = all_chunks(rest[first : first + rows])
                spill = pltpu.roll(jnp.where(lane < SPILL, value, 0.0), SPILL_LANE + SPILL * d, 1)
                value = jnp.where(lane < SPILL, 0.0, value) + spill
                last[y] = value if last[y] is None else last[y] + value
            mine[ROW_OF[d]] = tiles_of(main_rows)
        if g < len(GROUPS) - 1:
            return
        pad = [jnp.zeros((rows, AFFINE_LANE), jnp.float32)]
        pad.append(jnp.concatenate([affine[y] for y in range(side_y)], axis=0))
        pad.append(jnp.zeros((rows, LANES - AFFINE_LANE - affine.shape[2]), jnp.float32))
        mine[DIRS] = tiles_of(last) + jnp.concatenate(pad, axis=1)

    everyone = pl.ds(0, count_x)
    halves = (pl.ds(0, count_x // 2), pl.ds(count_x // 2, count_x - count_x // 2))

    def send(c, x, y, z, send_sem, recv_sem, other):
        first, end = CHUNKS[c]
        part = out.at[z, x, y, pl.ds(first, end - first)]
        return pltpu.make_async_remote_copy(
            src_ref=part,
            dst_ref=part,
            send_sem=send_sem,
            recv_sem=recv_sem,
            device_id=other,
            device_id_type=MESH,
        )

    def along(c, step):
        other = (jnp.clip(at_x + step, 0, count_x - 1), at_y, at_z)
        return send(c, at_x, at_y, at_z, line_send.at[c], line_recv.at[c, at_x], other)

    def along_in(c, x):
        return send(c, x, at_y, at_z, line_send.at[c], line_recv.at[c, x], (x, at_y, at_z))

    def along_sent(c):
        x = pl.ds(0, count_x - 1)
        return send(c, x, at_y, at_z, line_send.at[c], line_recv.at[c, 0], (at_x, at_y, at_z))

    def across(c, x, way):
        other = (at_x, near_y[way], at_z)
        return send(c, x, at_y, at_z, side_send.at[c, way], side_recv.at[c, way], other)

    def across_in(c, way):
        other = (at_x, near_y[way], at_z)
        return send(c, everyone, near_y[way], at_z, side_send.at[c, way], side_recv.at[c, way], other)

    def relay(c, way):
        other = (at_x, near_y[1 - way], at_z)
        sems = side_send.at[c, 2 + way], side_recv.at[c, 2 + way]
        return send(c, halves[way], near_y[way], at_z, *sems, other)

    def relay_in(c, way):
        other = (at_x, near_y[1 - way], at_z)
        sems = side_send.at[c, 2 + way], side_recv.at[c, 2 + way]
        return send(c, halves[way], near_y[2], at_z, *sems, other)

    def core_out(c, x, y, k):
        other = (at_x, at_y, (at_z + k) % count_z)
        return send(c, x, y, at_z, core_send.at[c, k - 1], core_recv.at[c, k - 1], other)

    def core_all(c, z, k):
        other = (at_x, at_y, (at_z + k) % count_z)
        every_y = pl.ds(0, count_y)
        return send(c, everyone, every_y, z, core_send.at[c, k - 1], core_recv.at[c, k - 1], other)

    def to_cores(c, x, y):
        for k in range(1, count_z):
            core_out(c, x, y, k).start()

    def spread(c, x):
        for way in (2, 0, 1) if c in DIRECT else (0, 1):
            across(c, x, way).start()
        to_cores(c, x, at_y)

    far_first = [k for far in range(count_x - 1, 0, -1) for k in (far, -far)]

    def others(body):
        for step in far_first[::-1]:

            @pl.when((at_x + step >= 0) & (at_x + step < count_x))
            def _(step=step):
                body(step)

    def line(c):
        for step in far_first:

            @pl.when((at_x + step >= 0) & (at_x + step < count_x))
            def _(step=step):
                along(c, step).start()

        spread(c, at_x)

    def side(c):
        def body(step):
            along_in(c, at_x + step).wait_recv()
            spread(c, at_x + step)

        others(body)

    def far(c):
        for way in range(2):
            across_in(c, way).wait_recv()
            if c not in DIRECT:
                relay(c, way).start()
            to_cores(c, everyone, near_y[way])

    def core(c):
        if c in DIRECT:
            across_in(c, 2).wait_recv()
        else:
            for way in range(2):
                relay_in(c, way).wait_recv()
        to_cores(c, everyone, near_y[2])

    solver = Solver(devices, bricks, blocks, turned_inverse)
    parts = out.reshape(count_z * count_x * count_y, DIRS + 1, 8, LANES)

    def load(c):
        for k in range(1, count_z):
            core_all(c, (at_z + count_z - k) % count_z, k).wait_recv()
        for r in range(*CHUNKS[c]):
            solver.load(parts, r)

    actions = {
        "here": here, "there": there_sums, "line": line, "side": side, "far": far, "core": core,
        "load": load,
    }
    for entry in SCHEDULE:
        name, g = entry.split()
        actions[name](int(g))

    for c in range(len(CHUNKS)):
        along_sent(c).wait_send()
        for way in range(2):
            across_in(c, way).wait_send()
        if c in DIRECT:
            across_in(c, 2).wait_send()
        else:
            for way in range(2):
                relay(c, way).wait_send()
        for k in range(1, count_z):
            core_all(c, at_z, k).wait_send()
    for i, piece in enumerate(pieces):
        if any(piece[3]):

            @pl.when(in_mesh(piece[3]))
            def _(i=i):
                halo(i).wait_send()

    solver.run(anchor, result_out, tiles)


def on_device(source_points, target_points, normals, weights, blocks, affines, anchor):
    bricks = source_points.shape[2:5]
    points = source_points.shape[5]
    devices = tuple(lax.axis_size(name) for name in AXES)
    grid = tuple(devices[axis] * bricks[axis] for axis in range(3))
    span = grid[0] * grid[1] * grid[2]
    chunks = points // LANES
    rows = chunks * bricks[2]
    assert bricks[0] == 1 and rows == 8 and devices[2] % 2 == 0 and devices[1] == 4
    assert bricks[1] * bricks[2] == 8
    assert span % (2 * LANES) == 0 and len(GROUPS[0]) * bricks[1] * rows == LANES

    def split(value):
        lead = value.shape[:-5]
        value = value.reshape(lead + (DIRS, bricks[1], bricks[2], chunks, LANES))
        return jnp.swapaxes(value, -3, -2)

    def filled(value):
        value = split(value)
        return value.reshape(value.shape[:-3] + (rows, LANES))

    params = functools.partial(pltpu.CompilerParams, vmem_limit_bytes=VMEM_BYTES)
    vmem = pl.BlockSpec(memory_space=pltpu.VMEM)
    anywhere = pl.BlockSpec(memory_space=pl.ANY)
    pieces = halo_pieces(bricks)
    remote = sum(any(piece[3]) for piece in pieces)
    dma = pltpu.SemaphoreType.DMA
    groups = len(GROUPS)
    own = (DIRS, bricks[1], rows, LANES)
    result = pl.pallas_call(
        functools.partial(step_kernel, devices, bricks),
        out_shape=jax.ShapeDtypeStruct(bricks[1:] + (24,), jnp.float32),
        in_specs=[anywhere] * 7,
        out_specs=vmem,
        scratch_shapes=[
            pltpu.SMEM((1,), jnp.int32),
            pltpu.SMEM(bricks[1:] + (DIRS,), jnp.int32),
            pltpu.VMEM(bricks[1:] + (12,), jnp.float32),
            pltpu.VMEM(
                (devices[2], devices[0], devices[1], DIRS + 1, 8, LANES), jnp.float32
            ),
            pltpu.VMEM((DIRS + 1, LANES // 4, 8, span // 2), jnp.float32),
            pltpu.VMEM((36, 8, span // 2), jnp.float32),
            pltpu.VMEM((span // 2, LANES), jnp.float32),
            dma((3,)),
            pltpu.VMEM((3,) + own, jnp.float32),
            pltpu.VMEM((3,) + own, jnp.float32),
            pltpu.VMEM(own, jnp.float32),
            pltpu.VMEM((3, DIRS, bricks[1], chunks, bricks[2], LANES), jnp.float32),
            pltpu.VMEM((10, len(GROUPS), LANES, LANES), jnp.float32),
            pltpu.VMEM((len(GROUPS), SUMS, 8, LANES), jnp.float32),
            dma((3,)),
            dma((len(pieces) - remote,)),
            dma((remote,)),
            dma((remote,)),
            dma((groups,)),
            dma((groups, devices[0])),
            dma((groups, 4)),
            dma((groups, 4)),
            dma((groups, devices[2] - 1)),
            dma((groups, devices[2] - 1)),
        ],
        compiler_params=params(collective_id=0, has_side_effects=True),
        name="step",
    )(
        anchor,
        jnp.transpose(blocks, (1, 2, 3, 0)).reshape(bricks[1], bricks[2], DIRS),
        jnp.transpose(affines, (1, 2, 3, 0)).reshape(bricks[1], bricks[2], 12),
        filled(source_points),
        split(target_points),
        filled(normals),
        filled(weights),
    )
    def placed(value):
        return jnp.transpose(value, (2, 0, 1)).reshape((12,) + bricks)

    return placed(result[..., :12]), placed(result[..., 12:])


def solution(mesh):
    points = P(None, None, "gx", "gy", "gz", None)
    tiles = P(None, "gx", "gy", "gz")
    return jax.shard_map(
        on_device,
        mesh=mesh,
        in_specs=(points, points, points, P(None, "gx", "gy", "gz", None), tiles, tiles, P()),
        out_specs=(tiles, tiles),
        check_vma=False,
    )
```

```python
import functools

import jax
import jax.numpy as jnp
from jax import lax
from jax.experimental import pallas as pl
from jax.experimental.pallas import tpu as pltpu
from jax.sharding import PartitionSpec as P

BLOCK = 256
ITERS = 10
SPACING = 0.5
DAMPING = 1.0
OFFSETS = (
    (1, 0, 0),
    (0, 1, 0),
    (0, 0, 1),
    (1, 1, -1),
    (1, -1, 1),
    (-1, 1, 1),
    (1, 1, 0),
    (1, 0, 1),
    (0, 1, 1),
    (1, 1, 1),
    (1, -1, 0),
    (0, 1, -1),
    (-1, 0, 1),
)
DIRS = len(OFFSETS)
LANES = 128
AXES = ("gx", "gy", "gz")
MESH = pl.DeviceIdType.MESH
VMEM_BYTES = 60 * 1024 * 1024

NORMAL_PAIRS = [(c, k) for c in range(3) for k in range(c, 3)]
POINT_PAIRS = [(e, k) for e in range(3) for k in range(e, 3)]
PAIR_ROWS = 96
THERE_ROWS = 36
SPILL = PAIR_ROWS + THERE_ROWS - LANES
SUMS = PAIR_ROWS + 2 * THERE_ROWS
SPILL_LANE = SPILL + THERE_ROWS
AFFINE_LANE = SPILL_LANE + SPILL * DIRS
SEND_ORDER = (1, 2, 8, 11, 3, 4, 9, 5, 7, 6, 12, 10)
GROUPS = ((1, 2, 8, 11), (3, 4, 5, 9), (7, 12, 6), (10, 0))
FLIPPED = 0
PLACED = tuple(tuple(-part for part in o) if d == FLIPPED else o for d, o in enumerate(OFFSETS))
ROW_OF = {d: place for place, d in enumerate(d for group in GROUPS for d in group)}
DIRECTION_OF = {place: d for d, place in ROW_OF.items()}
CHUNKS = ((0, 4), (4, 8), (8, 11), (11, DIRS + 1))
DIRECT = (0, 1, 2, 3)
LATE = (10,)
SCHEDULE = (
    "here 0", "here 1", "here 2", "there 0", "line 0", "late", "there 1",
    "line 1", "side 0", "there 2", "line 2", "here 3", "side 1", "there 3",
    "line 3", "side 2", "side 3", "far 0", "far 1", "core 0", "far 2",
    "core 1", "load 0", "far 3", "core 2", "load 1", "core 3", "load 2",
    "load 3",
)


def normal_pair(c, k):
    return NORMAL_PAIRS.index((min(c, k), max(c, k)))


def point_pair(e, k):
    return POINT_PAIRS.index((min(e, k), max(e, k)))


def moves(step, length):
    if step == 0:
        return [(slice(0, length), slice(0, length), 0)]
    if step > 0:
        return [
            (slice(step, length), slice(0, length - step), 0),
            (slice(0, step), slice(length - step, length), -1),
        ]
    return [
        (slice(0, length + step), slice(-step, length), 0),
        (slice(length + step, length), slice(0, -step), 1),
    ]


def halo_pieces(bricks):
    pieces = []
    for d in SEND_ORDER:
        dx, dy, dz = OFFSETS[d]
        for y_from, y_to, y_step in moves(dy, bricks[1]):
            for z_from, z_to, z_step in moves(dz, bricks[2]):
                pieces.append((d, (y_from, z_from), (y_to, z_to), (-dx, y_step, z_step)))
    return pieces


def all_of(conditions):
    result = None
    for condition in conditions:
        result = condition if result is None else jnp.logical_and(result, condition)
    return result


class Solver:
    def __init__(self, devices, bricks, blocks, turned):
        self.grid = tuple(devices[axis] * bricks[axis] for axis in range(3))
        self.bricks = bricks
        self.blocks = blocks
        self.turned = turned

    def load(self, parts, r):
        half = self.blocks.shape[3]
        many = LANES // 8
        d = DIRECTION_OF.get(r, DIRS)
        for start in range(0, half, LANES):
            first = parts[pl.ds(start // 8, many), r].reshape(LANES, LANES).T
            second = parts[pl.ds((half + start) // 8, many), r].reshape(LANES, LANES).T
            for i in range(LANES // 4):
                self.blocks[d, i, :, pl.ds(start, LANES)] = jnp.concatenate(
                    [first[4 * i : 4 * i + 4], second[4 * i : 4 * i + 4]], axis=0
                )

    def run(self, anchor, result_out, tiles):
        solve(self.grid, self.bricks, anchor, result_out, self.blocks, self.turned, tiles)


def solve(grid, bricks, anchor, result_out, blocks, turned, tiles):
    count_x, count_y, count_z = grid
    _, side_y, side_z = bricks
    half = blocks.shape[3]
    line = count_y * side_z
    plane = count_x * line
    lane = lax.broadcasted_iota(jnp.int32, (8, half), 1)
    sub = lax.broadcasted_iota(jnp.int32, (8, half), 0)
    column = sub % 4
    low = sub < 4

    def ahead(value, offset, sign=1):
        dx, dy, dz = (sign * part for part in offset)
        shift = dx * line + dy * side_z + dz
        result = pltpu.roll(value, (-shift) % half, 1)
        if dz:
            cross = shift + dz * (plane - side_z)
            other = pltpu.roll(value, (-cross) % half, 1)
            swapped = pltpu.roll(other, 4, 0)
            if plane != half:
                stays = (lane + cross >= 0) & (lane + cross < half)
                swapped = jnp.where(stays, other, swapped)
            edge = side_z - 1 if dz > 0 else 0
            result = jnp.where(lane % side_z == edge, swapped, result)
        return result

    def spread(value, e):
        return jnp.where(low, value[e : e + 1], value[4 + e : 5 + e])

    def butterfly(first, second, span):
        takes_first = (column & span) == 0
        return jnp.where(takes_first, first, pltpu.roll(second, span, 0)) + jnp.where(
            takes_first, pltpu.roll(first, 8 - span, 0), second
        )

    def columns_summed(four):
        return butterfly(butterfly(four[0], four[1], 1), butterfly(four[2], four[3], 1), 2)

    def total(terms):
        terms = list(terms)
        while len(terms) > 1:
            terms = [
                terms[i] + terms[i + 1] if i + 1 < len(terms) else terms[i]
                for i in range(0, len(terms), 2)
            ]
        return terms[0]

    JOINED = ((0, 1), (0, 2), (1, 2))

    def joins(vector):
        return [vector[c] + vector[k] for c, k in JOINED]

    def symmetric(d, e, vector, joined):
        shared = [
            blocks[d, normal_pair(*pair) * 4 + e] * value for pair, value in zip(JOINED, joined)
        ]
        own = [blocks[d, normal_pair(k, k) * 4 + e] * vector[k] for k in range(3)]
        return [own[k] + (shared[(0, 0, 1)[k]] + shared[(1, 2, 2)[k]]) for k in range(3)]

    def transposed(d, columns):
        rows = [symmetric(d, e, *columns[e]) for e in range(4)]
        return [total(rows[e][k] for e in range(4)) for k in range(3)]

    def operate(vector, shifted=False):
        columns = [[spread(vector[c], e) for c in range(3)] for e in range(4)]
        columns = [(column_e, joins(column_e)) for column_e in columns]
        result = transposed(DIRS, columns)
        sums = [[None] * 4 for _ in range(3)]
        back = [None] * 3
        for d, offset in enumerate(PLACED):
            near = [ahead(vector[k], offset) for k in range(3)]
            here = columns
            if shifted:
                near = [
                    near[k] + jnp.where(column == 3, SPACING * offset[k], 0.0) for k in range(3)
                ]
                edge = [columns[3][0][c] - SPACING * offset[c] for c in range(3)]
                here = columns[:3] + [(edge, joins(edge))]
            sent = transposed(d, here)
            joined = joins(near)
            for e in range(4):
                terms = symmetric(d, e, near, joined)
                for c in range(3):
                    sums[c][e] = terms[c] if sums[c][e] is None else sums[c][e] + terms[c]
            for k in range(3):
                term = ahead(sent[k], offset, -1)
                back[k] = term if back[k] is None else back[k] + term
        return [result[k] - back[k] - columns_summed(sums[k]) for k in range(3)]

    def rows_of(value):
        return [jnp.concatenate([value[f : f + 1], value[4 + f : 5 + f]], axis=0) for f in range(4)]

    both = []
    for g in range(THERE_ROWS // 4):
        value = blocks[DIRS, SPILL // 4 + g]
        for d, offset in enumerate(PLACED):
            group = PAIR_ROWS // 4 + g
            if group < LANES // 4:
                term = blocks[d, group]
            else:
                term = blocks[DIRS, SPILL_LANE // 4 + d]
            value = value + ahead(term, offset, -1)
        both.append(value)
    unit = [(column == k).astype(jnp.float32) for k in range(3)]
    affine = [blocks[DIRS, AFFINE_LANE // 4 + k] + unit[k] for k in range(3)]
    diagonal = []
    for s in range(6):
        edge = None
        for d, offset in enumerate(PLACED):
            term = ahead(blocks[d, s * 4 + 3], offset, -1)
            edge = term if edge is None else edge + term
        for e in range(4):
            term = total(blocks[d, s * 4 + e] for d in range(DIRS))
            edge = edge + jnp.where(column == e, spread(term, 3), 0.0)
        for e in range(3):
            value = spread(edge, e)
            for f in range(3):
                i = s * 6 + point_pair(e, f)
                value = jnp.where(column == f, spread(both[i // 4], i % 4), value)
            diagonal.append(value)
        diagonal.append(edge)
    brick_z = lane // plane + jnp.where(low, 0, half // plane)
    flat = lane % plane // side_z * count_z + brick_z * side_z + lane % side_z
    keep = (flat != anchor[0]).astype(jnp.float32)
    matrix = []
    for c in range(3):
        for e in range(4):
            row = []
            for k in range(3):
                value = diagonal[normal_pair(c, k) * 4 + e]
                if c == k:
                    eye = (column == e).astype(jnp.float32)
                    damped = value + DAMPING * eye
                    blocks_value = keep * damped + (1.0 - keep) * eye
                else:
                    blocks_value = keep * value
                row.append(blocks_value)
            matrix.append(row)
    for i, value in enumerate(diagonal):
        blocks[DIRS, i] = value

    def reduce_own(d):
        for e in range(4):
            shared = [blocks[d, normal_pair(*pair) * 4 + e] for pair in JOINED]
            for k in range(3):
                own = normal_pair(k, k) * 4 + e
                both_shared = shared[(0, 0, 1)[k]] + shared[(1, 2, 2)[k]]
                blocks[d, own] = blocks[d, own] - both_shared

    for d in range(DIRS + 1):
        reduce_own(d)
    rhs = [-(keep * value) for value in operate(affine, True)]
    for s, (c, k) in enumerate(NORMAL_PAIRS):
        if c == k:
            for e in range(4):
                value = blocks[DIRS, s * 4 + e]
                blocks[DIRS, s * 4 + e] = value + DAMPING * (column == e).astype(jnp.float32)
    for pivot in range(12):
        c, e = divmod(pivot, 4)
        here = matrix[pivot]
        factor = 1.0 / spread(here[c], e)
        at_pivot = column == e
        scaled = [here[k] * factor for k in range(3)]
        scaled[c] = jnp.where(at_pivot, factor, scaled[c])
        for a in range(12):
            if a == pivot:
                matrix[a] = scaled
            else:
                row = list(matrix[a])
                entry = spread(row[c], e)
                row[c] = jnp.where(at_pivot, 0.0, row[c])
                matrix[a] = [row[k] - entry * scaled[k] for k in range(3)]
    for a in range(12):
        for k in range(3):
            turned[a * 3 + k] = matrix[a][k]

    def precondition(vector):
        spreads = [[spread(vector[c], e) for e in range(4)] for c in range(3)]
        return [
            total(
                turned[(4 * c + e) * 3 + k] * spreads[c][e] for c in range(3) for e in range(4)
            )
            for k in range(3)
        ]

    def dot(left, right):
        value = total(left[k] * right[k] for k in range(3))
        value = total(value[:, start : start + LANES] for start in range(0, half, LANES))
        for span in (4, 2, 1):
            value = value + pltpu.roll(value, span, 0)
        return jnp.sum(value, axis=1, keepdims=True)

    first = precondition(rhs)

    def step(_, carry):
        update, residual, direction, inner_now = carry
        along = [keep * value for value in operate(direction)]
        alpha = inner_now / dot(direction, along)
        update = [update[k] + alpha * direction[k] for k in range(3)]
        residual = [residual[k] - alpha * along[k] for k in range(3)]
        scaled = precondition(residual)
        inner_next = dot(residual, scaled)
        beta = inner_next / inner_now
        direction = [scaled[k] + beta * direction[k] for k in range(3)]
        return update, residual, direction, inner_next

    start = ([jnp.zeros_like(value) for value in rhs], rhs, first, dot(rhs, first))
    update, residual, _, _ = lax.fori_loop(0, ITERS, step, start)

    at_x, at_y, at_z = (lax.axis_index(name) for name in AXES)
    bricks_half = half // plane
    upper = at_z // bricks_half
    base = (at_z - upper * bricks_half) * plane + at_x * line + at_y * side_y * side_z
    chosen = [jnp.where(upper == 0, v[:4], v[4:]) for v in update + residual]
    chosen.append(jnp.zeros((LANES - 24, half), jnp.float32))
    tall = jnp.concatenate(chosen, axis=0)
    for start in range(0, half, LANES):
        tiles[pl.ds(start, LANES), :] = tall[:, start : start + LANES].T
    rows = tiles[pl.ds(pl.multiple_of(base, 8), side_y * side_z), :]
    for y in range(side_y):
        row = rows[y * side_z : (y + 1) * side_z]
        result_out[y] = row[:, :24]


def step_kernel(
    devices, bricks,
    anchor_in, count_in, affine_in, source, target, normal, weight,
    result_out,
    anchor, count, affine, out, blocks, turned_inverse, tiles, small_sem,
    own_q, own_p, own_n, own_w, sent_w, flip_p, flip_n, flip_w, there, turned, acc,
    load_sem, stay_sem, halo_send, halo_recv,
    flip_send, flip_recv, sent, line_recv, side_recv, core_recv,
):
    count_x, count_y, count_z = devices
    _, side_y, side_z = bricks
    at = tuple(lax.axis_index(name) for name in AXES)
    at_x, at_y, at_z = at
    pieces = halo_pieces(bricks)
    leaving = [i for i, piece in enumerate(pieces) if any(piece[3])]
    staying = [i for i, piece in enumerate(pieces) if not any(piece[3])]
    chunks = source.shape[3] // side_z

    def in_mesh(offset):
        return all_of(
            [
                (at[axis] + step >= 0) & (at[axis] + step < devices[axis])
                for axis, step in enumerate(offset)
                if step
            ]
        )

    def beside(offset):
        return tuple(
            jnp.clip(at[axis] + step, 0, devices[axis] - 1) if step else at[axis]
            for axis, step in enumerate(offset)
        )

    near_y = [at_y + 1 - 2 * (at_y % 2), (at_y + 2) % count_y]
    near_y.append((near_y[0] + 2) % count_y)

    small = (
        pltpu.make_async_copy(count_in, count, small_sem.at[0]),
        pltpu.make_async_copy(affine_in, affine, small_sem.at[1]),
        pltpu.make_async_copy(anchor_in, anchor, small_sem.at[2]),
    )
    for copy in small:
        copy.start()

    load_target = pltpu.make_async_copy(target, own_q, load_sem.at[3])
    load_target.start()
    loads = (
        pltpu.make_async_copy(source, own_p, load_sem.at[0]),
        pltpu.make_async_copy(normal, own_n, load_sem.at[1]),
        pltpu.make_async_copy(weight, own_w, load_sem.at[2]),
    )
    for copy in loads:
        copy.start()

    for ref in (flip_p, flip_n, flip_w):
        ref[...] = jnp.zeros_like(ref)
    zeros = jnp.zeros(there.shape[2:], jnp.float32)
    for c in range(3):
        for d in range(DIRS):
            there[c, d] = zeros

    acc[...] = jnp.zeros_like(acc)

    barrier = pltpu.get_barrier_semaphore()
    steps = {piece[3] for piece in pieces if any(piece[3])}
    steps |= {tuple(-s for s in step) for step in steps}
    steps |= {(k, 0, 0) for k in range(1 - count_x, count_x) if k}
    steps = sorted(steps)
    expected = 0
    for step in steps:
        there_is = in_mesh(step)

        @pl.when(there_is)
        def _(step=step):
            pl.semaphore_signal(barrier, inc=1, device_id=beside(step), device_id_type=MESH)

        expected = expected + there_is.astype(jnp.int32)
    for other in near_y:
        pl.semaphore_signal(barrier, inc=1, device_id=(at_x, other, at_z), device_id_type=MESH)
    for k in range(1, count_z):
        pl.semaphore_signal(
            barrier, inc=1, device_id=(at_x, at_y, (at_z + k) % count_z), device_id_type=MESH
        )
    pl.semaphore_wait(barrier, expected + (3 + count_z - 1))

    def spot(ref, d, where):
        return ref.at[:, d, where[0], :, where[1], :]

    def halo(i):
        d, start, end, step = pieces[i]
        return pltpu.make_async_remote_copy(
            src_ref=spot(own_q, d, start),
            dst_ref=spot(there, d, end),
            send_sem=halo_send.at[leaving.index(i)],
            recv_sem=halo_recv.at[leaving.index(i)],
            device_id=beside(step),
            device_id_type=MESH,
        )

    def stay(i):
        d, start, end, _ = pieces[i]
        return pltpu.make_async_copy(spot(own_q, d, start), spot(there, d, end), stay_sem.at[staying.index(i)])

    def send_targets(late):
        for i, piece in enumerate(pieces):
            if (piece[0] in LATE) != late:
                continue
            if any(piece[3]):

                @pl.when(in_mesh(piece[3]))
                def _(i=i):
                    halo(i).start()

            else:
                stay(i).start()

    load_target.wait()
    send_targets(False)

    inside = {}
    for axis in range(3):
        length = devices[axis] * bricks[axis]
        for place in range(bricks[axis]):
            for step in (-1, 1):
                ahead = at[axis] * bricks[axis] + place + step
                inside[axis, place, step] = ((ahead >= 0) & (ahead < length)).astype(jnp.int32)

    for copy in small:
        copy.wait()
    rows = chunks * side_z
    sub = lax.broadcasted_iota(jnp.int32, (rows, LANES), 0)
    lane = lax.broadcasted_iota(jnp.int32, (rows, LANES), 1)
    point = lane + LANES * (sub // side_z)

    def live_weight(d, y):
        limit = None
        for z in range(side_z):
            value = count[y, z, d] * BLOCK
            for axis, place in enumerate((0, y, z)):
                if OFFSETS[d][axis]:
                    value = value * inside[axis, place, OFFSETS[d][axis]]
            limit = value if limit is None else jnp.where(sub % side_z == z, value, limit)
        return jnp.where(point < limit, own_w[d, y], 0.0)

    for copy in loads:
        copy.wait()
    for y in range(side_y):
        sent_w[y] = live_weight(FLIPPED, y)

    def flip(i):
        start, end = (
            (own_p.at[:, FLIPPED], flip_p),
            (own_n.at[:, FLIPPED], flip_n),
            (sent_w, flip_w),
        )[i]
        return pltpu.make_async_remote_copy(
            src_ref=start,
            dst_ref=end,
            send_sem=flip_send.at[i],
            recv_sem=flip_recv.at[i],
            device_id=beside((1, 0, 0)),
            device_id_type=MESH,
        )

    @pl.when(at_x < count_x - 1)
    def _():
        for i in range(3):
            flip(i).start()

    own_q_rows = own_q.reshape(3, DIRS, side_y, rows, LANES)

    def local(c, d, y):
        return own_q_rows[c, d, y] if d == FLIPPED else own_p[c, d, y]

    def ahead_of(c, d, y):
        return flip_p[c, y] if d == FLIPPED else there_rows[c, d, y]

    def normal_of(c, d, y):
        return flip_n[c, y] if d == FLIPPED else own_n[c, d, y]

    def weight_of(d, y):
        return flip_w[y] if d == FLIPPED else live_weight(d, y)

    def turn(parts):
        missing = LANES - rows * len(parts)
        if missing:
            parts = parts + [jnp.zeros((missing, LANES), jnp.float32)]
        return jnp.concatenate(parts, axis=0).T

    step = 32

    def summed(g, kinds):
        def body(chunk, carry):
            spots = pl.ds(pl.multiple_of(chunk * step, step), step)
            p = [turned[c, g, spots, :] for c in range(3)] + [None]
            q = [turned[7 + c, g, spots, :] for c in range(3)] + [None] if kinds == "there" else None
            n = [turned[3 + c, g, spots, :] for c in range(3)]
            w = turned[6, g, spots, :]

            def times(left, right):
                if left is None:
                    return right
                return left if right is None else left * right

            def add(row, value):
                acc[g, row] += jnp.sum(value.reshape(step // 8, 8, LANES), axis=0)

            wn = [w * n[c] for c in range(3)]
            weighted = [wn[c] * n[k] for c, k in NORMAL_PAIRS]
            if kinds == "here":
                for e in range(4):
                    for s in range(6):
                        add(s * 16 + e * 4 + 3, times(weighted[s], p[e]))
                for place, (e, k) in enumerate(POINT_PAIRS):
                    product = p[e] * p[k]
                    for s in range(6):
                        add(PAIR_ROWS + THERE_ROWS + s * 6 + place, weighted[s] * product)
            else:
                for e in range(4):
                    for k in range(3):
                        product = times(p[e], q[k])
                        for s in range(6):
                            add(s * 16 + e * 4 + k, weighted[s] * product)
                for place, (e, k) in enumerate(POINT_PAIRS):
                    product = q[e] * q[k]
                    for s in range(6):
                        add(PAIR_ROWS + s * 6 + place, weighted[s] * product)
            return carry

        lax.fori_loop(0, LANES // step, body, 0)

    def here(g):
        group = GROUPS[g]
        if FLIPPED in group:

            @pl.when(at_x > 0)
            def _():
                for i in range(3):
                    flip(i).wait_recv()

        for c in range(3):
            turned[c, g] = turn([local(c, d, y) for d in group for y in range(side_y)])
            turned[3 + c, g] = turn([normal_of(c, d, y) for d in group for y in range(side_y)])
        turned[6, g] = turn([weight_of(d, y) for d in group for y in range(side_y)])
        summed(g, "here")

    there_rows = there.reshape(3, DIRS, side_y, rows, LANES)
    last = [None] * side_y
    mine = out.at[at_z, at_x, at_y]

    def tiles_of(values):
        result = values[0]
        for y in range(1, side_y):
            result = jnp.where(sub // side_z == y, values[y], result)
        return result

    def there_sums(g):
        group = GROUPS[g]
        for i, piece in enumerate(pieces):
            if piece[0] in group:
                if any(piece[3]):

                    @pl.when(in_mesh(tuple(-s for s in piece[3])))
                    def _(i=i):
                        halo(i).wait_recv()

                else:
                    stay(i).wait()
        for c in range(3):
            turned[7 + c, g] = turn([ahead_of(c, d, y) for d in group for y in range(side_y)])
        summed(g, "there")
        whole = [jnp.sum(acc[g, r : r + 8], axis=1) for r in range(0, SUMS, 8)]
        main = jnp.concatenate(whole[: LANES // 8], axis=0).T
        rest = whole[LANES // 8 :] + [jnp.zeros((2 * LANES - SUMS, LANES), jnp.float32)]
        rest = jnp.concatenate(rest, axis=0).T

        def all_chunks(value):
            span = rows // 2
            while span >= side_z:
                value = value + pltpu.roll(value, span, 0)
                span //= 2
            return value

        for place, d in enumerate(group):
            main_rows = []
            for y in range(side_y):
                first = (place * side_y + y) * rows
                main_rows.append(all_chunks(main[first : first + rows]))
                value = all_chunks(rest[first : first + rows])
                spill = pltpu.roll(jnp.where(lane < SPILL, value, 0.0), SPILL_LANE + SPILL * d, 1)
                value = jnp.where(lane < SPILL, 0.0, value) + spill
                last[y] = value if last[y] is None else last[y] + value
            mine[ROW_OF[d]] = tiles_of(main_rows)
        if g < len(GROUPS) - 1:
            return
        pad = [jnp.zeros((rows, AFFINE_LANE), jnp.float32)]
        pad.append(jnp.concatenate([affine[y] for y in range(side_y)], axis=0))
        pad.append(jnp.zeros((rows, LANES - AFFINE_LANE - affine.shape[2]), jnp.float32))
        mine[DIRS] = tiles_of(last) + jnp.concatenate(pad, axis=1)

    everyone = pl.ds(0, count_x)
    halves = (pl.ds(0, count_x // 2), pl.ds(count_x // 2, count_x - count_x // 2))

    def send(c, x, y, z, send_sem, recv_sem, other):
        first, end = CHUNKS[c]
        part = out.at[z, x, y, pl.ds(first, end - first)]
        return pltpu.make_async_remote_copy(
            src_ref=part,
            dst_ref=part,
            send_sem=send_sem,
            recv_sem=recv_sem,
            device_id=other,
            device_id_type=MESH,
        )

    def along(c, step):
        other = (jnp.clip(at_x + step, 0, count_x - 1), at_y, at_z)
        return send(c, at_x, at_y, at_z, sent.at[0], line_recv.at[c, at_x], other)

    def along_in(c, x):
        return send(c, x, at_y, at_z, sent.at[0], line_recv.at[c, x], (x, at_y, at_z))

    def across(c, x, way):
        other = (at_x, near_y[way], at_z)
        return send(c, x, at_y, at_z, sent.at[1], side_recv.at[c, way], other)

    def across_in(c, way):
        other = (at_x, near_y[way], at_z)
        return send(c, everyone, near_y[way], at_z, sent.at[1], side_recv.at[c, way], other)

    def relay(c, way):
        other = (at_x, near_y[1 - way], at_z)
        sems = sent.at[3 + way], side_recv.at[c, 2 + way]
        return send(c, halves[way], near_y[way], at_z, *sems, other)

    def relay_in(c, way):
        other = (at_x, near_y[1 - way], at_z)
        sems = sent.at[3 + way], side_recv.at[c, 2 + way]
        return send(c, halves[way], near_y[2], at_z, *sems, other)

    def core_out(c, x, y, k):
        other = (at_x, at_y, (at_z + k) % count_z)
        return send(c, x, y, at_z, sent.at[2], core_recv.at[c, k - 1], other)

    def core_all(c, z, k):
        other = (at_x, at_y, (at_z + k) % count_z)
        every_y = pl.ds(0, count_y)
        return send(c, everyone, every_y, z, sent.at[2], core_recv.at[c, k - 1], other)

    def to_cores(c, x, y):
        for k in range(1, count_z):
            core_out(c, x, y, k).start()

    def spread(c, x):
        for way in (2, 0, 1) if c in DIRECT else (0, 1):
            across(c, x, way).start()
        to_cores(c, x, at_y)

    far_first = [k for far in range(count_x - 1, 0, -1) for k in (far, -far)]

    def others(body):
        for step in far_first[::-1]:

            @pl.when((at_x + step >= 0) & (at_x + step < count_x))
            def _(step=step):
                body(step)

    def line(c):
        for step in far_first:

            @pl.when((at_x + step >= 0) & (at_x + step < count_x))
            def _(step=step):
                along(c, step).start()

        spread(c, at_x)

    def side(c):
        def body(step):
            along_in(c, at_x + step).wait_recv()
            spread(c, at_x + step)

        others(body)

    def far(c):
        for way in range(2):
            across_in(c, way).wait_recv()
            if c not in DIRECT:
                relay(c, way).start()
            to_cores(c, everyone, near_y[way])

    def core(c):
        if c in DIRECT:
            across_in(c, 2).wait_recv()
        else:
            for way in range(2):
                relay_in(c, way).wait_recv()
        to_cores(c, everyone, near_y[2])

    solver = Solver(devices, bricks, blocks, turned_inverse)
    parts = out.reshape(count_z * count_x * count_y, DIRS + 1, 8, LANES)

    def load(c):
        for k in range(1, count_z):
            core_all(c, (at_z + count_z - k) % count_z, k).wait_recv()
        for r in range(*CHUNKS[c]):
            solver.load(parts, r)

    actions = {
        "here": here, "there": there_sums, "line": line, "side": side, "far": far, "core": core,
        "load": load,
    }
    for entry in SCHEDULE:
        if entry == "late":
            send_targets(True)
            continue
        name, g = entry.split()
        actions[name](int(g))

    def all_sent(kind, region):
        pltpu.make_async_remote_copy(
            src_ref=region,
            dst_ref=region,
            send_sem=sent.at[kind],
            recv_sem=core_recv.at[0, 0],
            device_id=(at_x, at_y, (at_z + 1) % count_z),
            device_id_type=MESH,
        ).wait_send()

    assert len(DIRECT) == len(CHUNKS)
    all_sent(0, out.at[at_z, pl.ds(0, count_x - 1), 0])
    all_sent(1, out.at[at_z, :, pl.ds(0, 3)])
    all_sent(2, out.at[pl.ds(0, count_z - 1)])
    for i, piece in enumerate(pieces):
        if any(piece[3]):

            @pl.when(in_mesh(piece[3]))
            def _(i=i):
                halo(i).wait_send()

    @pl.when(at_x < count_x - 1)
    def _():
        for i in range(3):
            flip(i).wait_send()

    solver.run(anchor, result_out, tiles)


def on_device(source_points, target_points, normals, weights, blocks, affines, anchor):
    bricks = source_points.shape[2:5]
    points = source_points.shape[5]
    devices = tuple(lax.axis_size(name) for name in AXES)
    grid = tuple(devices[axis] * bricks[axis] for axis in range(3))
    span = grid[0] * grid[1] * grid[2]
    chunks = points // LANES
    rows = chunks * bricks[2]
    assert bricks[0] == 1 and rows == 8 and devices[2] % 2 == 0 and devices[1] == 4
    assert bricks[1] * bricks[2] == 8
    assert span % (2 * LANES) == 0 and len(GROUPS[0]) * bricks[1] * rows == LANES

    def split(value):
        lead = value.shape[:-5]
        value = value.reshape(lead + (DIRS, bricks[1], bricks[2], chunks, LANES))
        return jnp.swapaxes(value, -3, -2)

    def filled(value):
        value = split(value)
        return value.reshape(value.shape[:-3] + (rows, LANES))

    params = functools.partial(pltpu.CompilerParams, vmem_limit_bytes=VMEM_BYTES)
    vmem = pl.BlockSpec(memory_space=pltpu.VMEM)
    anywhere = pl.BlockSpec(memory_space=pl.ANY)
    pieces = halo_pieces(bricks)
    remote = sum(any(piece[3]) for piece in pieces)
    dma = pltpu.SemaphoreType.DMA
    groups = len(GROUPS)
    own = (DIRS, bricks[1], rows, LANES)
    result = pl.pallas_call(
        functools.partial(step_kernel, devices, bricks),
        out_shape=jax.ShapeDtypeStruct(bricks[1:] + (24,), jnp.float32),
        in_specs=[anywhere] * 7,
        out_specs=vmem,
        scratch_shapes=[
            pltpu.SMEM((1,), jnp.int32),
            pltpu.SMEM(bricks[1:] + (DIRS,), jnp.int32),
            pltpu.VMEM(bricks[1:] + (12,), jnp.float32),
            pltpu.VMEM(
                (devices[2], devices[0], devices[1], DIRS + 1, 8, LANES), jnp.float32
            ),
            pltpu.VMEM((DIRS + 1, LANES // 4, 8, span // 2), jnp.float32),
            pltpu.VMEM((36, 8, span // 2), jnp.float32),
            pltpu.VMEM((span // 2, LANES), jnp.float32),
            dma((3,)),
            pltpu.VMEM((3, DIRS, bricks[1], chunks, bricks[2], LANES), jnp.float32),
            pltpu.VMEM((3,) + own, jnp.float32),
            pltpu.VMEM((3,) + own, jnp.float32),
            pltpu.VMEM(own, jnp.float32),
            pltpu.VMEM(own[1:], jnp.float32),
            pltpu.VMEM((3,) + own[1:], jnp.float32),
            pltpu.VMEM((3,) + own[1:], jnp.float32),
            pltpu.VMEM(own[1:], jnp.float32),
            pltpu.VMEM((3, DIRS, bricks[1], chunks, bricks[2], LANES), jnp.float32),
            pltpu.VMEM((10, len(GROUPS), LANES, LANES), jnp.float32),
            pltpu.VMEM((len(GROUPS), SUMS, 8, LANES), jnp.float32),
            dma((4,)),
            dma((len(pieces) - remote,)),
            dma((remote,)),
            dma((remote,)),
            dma((3,)),
            dma((3,)),
            dma((3,)),
            dma((groups, devices[0])),
            dma((groups, 3)),
            dma((groups, devices[2] - 1)),
        ],
        compiler_params=params(collective_id=0, has_side_effects=True),
        name="step",
    )(
        anchor,
        jnp.transpose(blocks, (1, 2, 3, 0)).reshape(bricks[1], bricks[2], DIRS),
        jnp.transpose(affines, (1, 2, 3, 0)).reshape(bricks[1], bricks[2], 12),
        filled(source_points),
        split(target_points),
        filled(normals),
        filled(weights),
    )
    def placed(value):
        return jnp.transpose(value, (2, 0, 1)).reshape((12,) + bricks)

    return placed(result[..., :12]), placed(result[..., 12:])


def solution(mesh):
    points = P(None, None, "gx", "gy", "gz", None)
    tiles = P(None, "gx", "gy", "gz")
    return jax.shard_map(
        on_device,
        mesh=mesh,
        in_specs=(points, points, points, P(None, "gx", "gy", "gz", None), tiles, tiles, P()),
        out_specs=(tiles, tiles),
        check_vma=False,
    )
```

```python
import functools

import jax
import jax.numpy as jnp
from jax import lax
from jax.experimental import pallas as pl
from jax.experimental.pallas import tpu as pltpu
from jax.sharding import PartitionSpec as P

BLOCK = 256
ITERS = 10
SPACING = 0.5
DAMPING = 1.0
OFFSETS = (
    (1, 0, 0),
    (0, 1, 0),
    (0, 0, 1),
    (1, 1, -1),
    (1, -1, 1),
    (-1, 1, 1),
    (1, 1, 0),
    (1, 0, 1),
    (0, 1, 1),
    (1, 1, 1),
    (1, -1, 0),
    (0, 1, -1),
    (-1, 0, 1),
)
DIRS = len(OFFSETS)
LANES = 128
AXES = ("gx", "gy", "gz")
MESH = pl.DeviceIdType.MESH
VMEM_BYTES = 60 * 1024 * 1024

NORMAL_PAIRS = [(c, k) for c in range(3) for k in range(c, 3)]
POINT_PAIRS = [(e, k) for e in range(3) for k in range(e, 3)]
PAIR_ROWS = 96
THERE_ROWS = 36
SPILL = PAIR_ROWS + THERE_ROWS - LANES
SUMS = PAIR_ROWS + 2 * THERE_ROWS
SPILL_LANE = SPILL + THERE_ROWS
AFFINE_LANE = SPILL_LANE + SPILL * DIRS
SEND_ORDER = (1, 2, 8, 11, 3, 4, 9, 5, 7, 6, 12, 10)
GROUPS = ((1, 2, 8, 11), (3, 4, 5, 9), (7, 12, 6), (10, 0))
FLIPPED = 0
PLACED = tuple(tuple(-part for part in o) if d == FLIPPED else o for d, o in enumerate(OFFSETS))
ROW_OF = {d: place for place, d in enumerate(d for group in GROUPS for d in group)}
DIRECTION_OF = {place: d for d, place in ROW_OF.items()}
CHUNKS = ((0, 4), (4, 8), (8, 11), (11, DIRS + 1))
DIRECT = (0, 1, 2, 3)
LATE = (10,)
SCHEDULE = (
    "here 0", "here 1", "here 2", "there 0", "line 0", "late", "there 1",
    "line 1", "side 0", "there 2", "line 2", "here 3", "side 1", "there 3",
    "line 3", "side 2", "side 3", "far 0", "far 1", "core 0", "far 2",
    "core 1", "load 0", "far 3", "core 2", "load 1", "core 3", "load 2",
    "load 3",
)


def normal_pair(c, k):
    return NORMAL_PAIRS.index((min(c, k), max(c, k)))


def point_pair(e, k):
    return POINT_PAIRS.index((min(e, k), max(e, k)))


def moves(step, length):
    if step == 0:
        return [(slice(0, length), slice(0, length), 0)]
    if step > 0:
        return [
            (slice(step, length), slice(0, length - step), 0),
            (slice(0, step), slice(length - step, length), -1),
        ]
    return [
        (slice(0, length + step), slice(-step, length), 0),
        (slice(length + step, length), slice(0, -step), 1),
    ]


def halo_pieces(bricks):
    pieces = []
    for d in SEND_ORDER:
        dx, dy, dz = OFFSETS[d]
        for y_from, y_to, y_step in moves(dy, bricks[1]):
            for z_from, z_to, z_step in moves(dz, bricks[2]):
                pieces.append((d, (y_from, z_from), (y_to, z_to), (-dx, y_step, z_step)))
    return pieces


def size_of(piece):
    _, (y, z), _, _ = piece
    return (y.stop - y.start) * (z.stop - z.start)


def arrivals(pieces):
    result = {}
    for piece in pieces:
        if any(piece[3]):
            key = next(g for g, group in enumerate(GROUPS) if piece[0] in group), piece[3]
            result[key] = result.get(key, 0) + size_of(piece)
    return result


def box_of(size, bricks):
    return next(
        (a, b, c)
        for a in range(1, DIRS + 1)
        for b in range(1, bricks[1] + 1)
        for c in range(1, bricks[2] + 1)
        if a * b * c == size
    )


def all_of(conditions):
    result = None
    for condition in conditions:
        result = condition if result is None else jnp.logical_and(result, condition)
    return result


class Solver:
    def __init__(self, devices, bricks, blocks, turned):
        self.grid = tuple(devices[axis] * bricks[axis] for axis in range(3))
        self.bricks = bricks
        self.blocks = blocks
        self.turned = turned

    def load(self, parts, r):
        half = self.blocks.shape[3]
        many = LANES // 8
        d = DIRECTION_OF.get(r, DIRS)
        for start in range(0, half, LANES):
            first = parts[pl.ds(start // 8, many), r].reshape(LANES, LANES).T
            second = parts[pl.ds((half + start) // 8, many), r].reshape(LANES, LANES).T
            for i in range(LANES // 4):
                self.blocks[d, i, :, pl.ds(start, LANES)] = jnp.concatenate(
                    [first[4 * i : 4 * i + 4], second[4 * i : 4 * i + 4]], axis=0
                )

    def run(self, anchor, result_out, tiles):
        solve(self.grid, self.bricks, anchor, result_out, self.blocks, self.turned, tiles)


def solve(grid, bricks, anchor, result_out, blocks, turned, tiles):
    count_x, count_y, count_z = grid
    _, side_y, side_z = bricks
    half = blocks.shape[3]
    line = count_y * side_z
    plane = count_x * line
    lane = lax.broadcasted_iota(jnp.int32, (8, half), 1)
    sub = lax.broadcasted_iota(jnp.int32, (8, half), 0)
    column = sub % 4
    low = sub < 4

    def ahead(value, offset, sign=1):
        dx, dy, dz = (sign * part for part in offset)
        shift = dx * line + dy * side_z + dz
        result = pltpu.roll(value, (-shift) % half, 1)
        if dz:
            cross = shift + dz * (plane - side_z)
            other = pltpu.roll(value, (-cross) % half, 1)
            swapped = pltpu.roll(other, 4, 0)
            if plane != half:
                stays = (lane + cross >= 0) & (lane + cross < half)
                swapped = jnp.where(stays, other, swapped)
            edge = side_z - 1 if dz > 0 else 0
            result = jnp.where(lane % side_z == edge, swapped, result)
        return result

    def spread(value, e):
        return jnp.where(low, value[e : e + 1], value[4 + e : 5 + e])

    def butterfly(first, second, span):
        takes_first = (column & span) == 0
        return jnp.where(takes_first, first, pltpu.roll(second, span, 0)) + jnp.where(
            takes_first, pltpu.roll(first, 8 - span, 0), second
        )

    def columns_summed(four):
        return butterfly(butterfly(four[0], four[1], 1), butterfly(four[2], four[3], 1), 2)

    def total(terms):
        terms = list(terms)
        while len(terms) > 1:
            terms = [
                terms[i] + terms[i + 1] if i + 1 < len(terms) else terms[i]
                for i in range(0, len(terms), 2)
            ]
        return terms[0]

    JOINED = ((0, 1), (0, 2), (1, 2))

    def joins(vector):
        return [vector[c] + vector[k] for c, k in JOINED]

    def symmetric(d, e, vector, joined):
        shared = [
            blocks[d, normal_pair(*pair) * 4 + e] * value for pair, value in zip(JOINED, joined)
        ]
        own = [blocks[d, normal_pair(k, k) * 4 + e] * vector[k] for k in range(3)]
        return [own[k] + (shared[(0, 0, 1)[k]] + shared[(1, 2, 2)[k]]) for k in range(3)]

    def transposed(d, columns):
        rows = [symmetric(d, e, *columns[e]) for e in range(4)]
        return [total(rows[e][k] for e in range(4)) for k in range(3)]

    def operate(vector, shifted=False):
        columns = [[spread(vector[c], e) for c in range(3)] for e in range(4)]
        columns = [(column_e, joins(column_e)) for column_e in columns]
        result = transposed(DIRS, columns)
        sums = [[None] * 4 for _ in range(3)]
        back = [None] * 3
        for d, offset in enumerate(PLACED):
            near = [ahead(vector[k], offset) for k in range(3)]
            here = columns
            if shifted:
                near = [
                    near[k] + jnp.where(column == 3, SPACING * offset[k], 0.0) for k in range(3)
                ]
                edge = [columns[3][0][c] - SPACING * offset[c] for c in range(3)]
                here = columns[:3] + [(edge, joins(edge))]
            sent = transposed(d, here)
            joined = joins(near)
            for e in range(4):
                terms = symmetric(d, e, near, joined)
                for c in range(3):
                    sums[c][e] = terms[c] if sums[c][e] is None else sums[c][e] + terms[c]
            for k in range(3):
                term = ahead(sent[k], offset, -1)
                back[k] = term if back[k] is None else back[k] + term
        return [result[k] - back[k] - columns_summed(sums[k]) for k in range(3)]

    def rows_of(value):
        return [jnp.concatenate([value[f : f + 1], value[4 + f : 5 + f]], axis=0) for f in range(4)]

    both = []
    for g in range(THERE_ROWS // 4):
        value = blocks[DIRS, SPILL // 4 + g]
        for d, offset in enumerate(PLACED):
            group = PAIR_ROWS // 4 + g
            if group < LANES // 4:
                term = blocks[d, group]
            else:
                term = blocks[DIRS, SPILL_LANE // 4 + d]
            value = value + ahead(term, offset, -1)
        both.append(value)
    unit = [(column == k).astype(jnp.float32) for k in range(3)]
    affine = [blocks[DIRS, AFFINE_LANE // 4 + k] + unit[k] for k in range(3)]
    diagonal = []
    for s in range(6):
        edge = None
        for d, offset in enumerate(PLACED):
            term = ahead(blocks[d, s * 4 + 3], offset, -1)
            edge = term if edge is None else edge + term
        for e in range(4):
            term = total(blocks[d, s * 4 + e] for d in range(DIRS))
            edge = edge + jnp.where(column == e, spread(term, 3), 0.0)
        for e in range(3):
            value = spread(edge, e)
            for f in range(3):
                i = s * 6 + point_pair(e, f)
                value = jnp.where(column == f, spread(both[i // 4], i % 4), value)
            diagonal.append(value)
        diagonal.append(edge)
    brick_z = lane // plane + jnp.where(low, 0, half // plane)
    flat = lane % plane // side_z * count_z + brick_z * side_z + lane % side_z
    keep = (flat != anchor[0]).astype(jnp.float32)
    matrix = []
    for c in range(3):
        for e in range(4):
            row = []
            for k in range(3):
                value = diagonal[normal_pair(c, k) * 4 + e]
                if c == k:
                    eye = (column == e).astype(jnp.float32)
                    damped = value + DAMPING * eye
                    blocks_value = keep * damped + (1.0 - keep) * eye
                else:
                    blocks_value = keep * value
                row.append(blocks_value)
            matrix.append(row)
    for i, value in enumerate(diagonal):
        blocks[DIRS, i] = value

    def reduce_own(d):
        for e in range(4):
            shared = [blocks[d, normal_pair(*pair) * 4 + e] for pair in JOINED]
            for k in range(3):
                own = normal_pair(k, k) * 4 + e
                both_shared = shared[(0, 0, 1)[k]] + shared[(1, 2, 2)[k]]
                blocks[d, own] = blocks[d, own] - both_shared

    for d in range(DIRS + 1):
        reduce_own(d)
    rhs = [-(keep * value) for value in operate(affine, True)]
    for s, (c, k) in enumerate(NORMAL_PAIRS):
        if c == k:
            for e in range(4):
                value = blocks[DIRS, s * 4 + e]
                blocks[DIRS, s * 4 + e] = value + DAMPING * (column == e).astype(jnp.float32)
    for pivot in range(12):
        c, e = divmod(pivot, 4)
        here = matrix[pivot]
        factor = 1.0 / spread(here[c], e)
        at_pivot = column == e
        scaled = [here[k] * factor for k in range(3)]
        scaled[c] = jnp.where(at_pivot, factor, scaled[c])
        for a in range(12):
            if a == pivot:
                matrix[a] = scaled
            else:
                row = list(matrix[a])
                entry = spread(row[c], e)
                row[c] = jnp.where(at_pivot, 0.0, row[c])
                matrix[a] = [row[k] - entry * scaled[k] for k in range(3)]
    for a in range(12):
        for k in range(3):
            turned[a * 3 + k] = matrix[a][k]

    def precondition(vector):
        spreads = [[spread(vector[c], e) for e in range(4)] for c in range(3)]
        return [
            total(
                turned[(4 * c + e) * 3 + k] * spreads[c][e] for c in range(3) for e in range(4)
            )
            for k in range(3)
        ]

    def dot(left, right):
        value = total(left[k] * right[k] for k in range(3))
        value = total(value[:, start : start + LANES] for start in range(0, half, LANES))
        for span in (4, 2, 1):
            value = value + pltpu.roll(value, span, 0)
        return jnp.sum(value, axis=1, keepdims=True)

    first = precondition(rhs)

    def step(_, carry):
        update, residual, direction, inner_now = carry
        along = [keep * value for value in operate(direction)]
        alpha = inner_now / dot(direction, along)
        update = [update[k] + alpha * direction[k] for k in range(3)]
        residual = [residual[k] - alpha * along[k] for k in range(3)]
        scaled = precondition(residual)
        inner_next = dot(residual, scaled)
        beta = inner_next / inner_now
        direction = [scaled[k] + beta * direction[k] for k in range(3)]
        return update, residual, direction, inner_next

    start = ([jnp.zeros_like(value) for value in rhs], rhs, first, dot(rhs, first))
    update, residual, _, _ = lax.fori_loop(0, ITERS, step, start)

    at_x, at_y, at_z = (lax.axis_index(name) for name in AXES)
    bricks_half = half // plane
    upper = at_z // bricks_half
    base = (at_z - upper * bricks_half) * plane + at_x * line + at_y * side_y * side_z
    chosen = [jnp.where(upper == 0, v[:4], v[4:]) for v in update + residual]
    chosen.append(jnp.zeros((LANES - 24, half), jnp.float32))
    tall = jnp.concatenate(chosen, axis=0)
    for start in range(0, half, LANES):
        tiles[pl.ds(start, LANES), :] = tall[:, start : start + LANES].T
    rows = tiles[pl.ds(pl.multiple_of(base, 8), side_y * side_z), :]
    for y in range(side_y):
        row = rows[y * side_z : (y + 1) * side_z]
        result_out[y] = row[:, :24]


def step_kernel(
    devices, bricks,
    anchor_in, count_in, affine_in, source, target, normal, weight,
    result_out,
    anchor, count, affine, out, blocks, turned_inverse, tiles, small_sem,
    own_q, own_p, own_n, own_w, sent_w, flip_p, flip_n, flip_w, there, turned, acc,
    load_sem, stay_sem, halo_send, halo_recv,
    flip_send, flip_recv, sent, line_recv, side_recv, core_recv,
):
    count_x, count_y, count_z = devices
    _, side_y, side_z = bricks
    at = tuple(lax.axis_index(name) for name in AXES)
    at_x, at_y, at_z = at
    pieces = halo_pieces(bricks)
    arrive = arrivals(pieces)
    arrive_at = list(arrive)
    staying = [i for i, piece in enumerate(pieces) if not any(piece[3])]
    chunks = source.shape[3] // side_z

    def in_mesh(offset):
        return all_of(
            [
                (at[axis] + step >= 0) & (at[axis] + step < devices[axis])
                for axis, step in enumerate(offset)
                if step
            ]
        )

    def beside(offset):
        return tuple(
            jnp.clip(at[axis] + step, 0, devices[axis] - 1) if step else at[axis]
            for axis, step in enumerate(offset)
        )

    near_y = [at_y + 1 - 2 * (at_y % 2), (at_y + 2) % count_y]
    near_y.append((near_y[0] + 2) % count_y)

    small = (
        pltpu.make_async_copy(count_in, count, small_sem.at[0]),
        pltpu.make_async_copy(affine_in, affine, small_sem.at[1]),
        pltpu.make_async_copy(anchor_in, anchor, small_sem.at[2]),
    )
    for copy in small:
        copy.start()

    load_target = pltpu.make_async_copy(target, own_q, load_sem.at[3])
    load_target.start()
    loads = (
        pltpu.make_async_copy(source, own_p, load_sem.at[0]),
        pltpu.make_async_copy(normal, own_n, load_sem.at[1]),
        pltpu.make_async_copy(weight, own_w, load_sem.at[2]),
    )
    for copy in loads:
        copy.start()

    for ref in (flip_p, flip_n, flip_w):
        ref[...] = jnp.zeros_like(ref)
    zeros = jnp.zeros(there.shape[2:], jnp.float32)
    for c in range(3):
        for d in range(DIRS):
            there[c, d] = zeros

    acc[...] = jnp.zeros_like(acc)

    barrier = pltpu.get_barrier_semaphore()
    steps = {piece[3] for piece in pieces if any(piece[3])}
    steps |= {tuple(-s for s in step) for step in steps}
    steps |= {(k, 0, 0) for k in range(1 - count_x, count_x) if k}
    steps = sorted(steps)
    expected = 0
    for step in steps:
        there_is = in_mesh(step)

        @pl.when(there_is)
        def _(step=step):
            pl.semaphore_signal(barrier, inc=1, device_id=beside(step), device_id_type=MESH)

        expected = expected + there_is.astype(jnp.int32)
    for other in near_y:
        pl.semaphore_signal(barrier, inc=1, device_id=(at_x, other, at_z), device_id_type=MESH)
    for k in range(1, count_z):
        pl.semaphore_signal(
            barrier, inc=1, device_id=(at_x, at_y, (at_z + k) % count_z), device_id_type=MESH
        )
    pl.semaphore_wait(barrier, expected + (3 + count_z - 1))

    def spot(ref, d, where):
        return ref.at[:, d, where[0], :, where[1], :]

    def halo(i):
        d, start, end, step = pieces[i]
        g = next(g for g, group in enumerate(GROUPS) if d in group)
        return pltpu.make_async_remote_copy(
            src_ref=spot(own_q, d, start),
            dst_ref=spot(there, d, end),
            send_sem=halo_send.at[arrive_at.index((g, step))],
            recv_sem=halo_recv.at[arrive_at.index((g, step))],
            device_id=beside(step),
            device_id_type=MESH,
        )

    def halo_bytes(size, leaves, arrives, step):
        a, b, c = box_of(size, bricks)
        box = (slice(None), slice(0, a), slice(0, b), slice(None), slice(0, c))
        return pltpu.make_async_remote_copy(
            src_ref=own_q.at[box],
            dst_ref=there.at[box],
            send_sem=halo_send.at[leaves],
            recv_sem=halo_recv.at[arrives],
            device_id=beside(step),
            device_id_type=MESH,
        )

    def stay(i):
        d, start, end, _ = pieces[i]
        return pltpu.make_async_copy(spot(own_q, d, start), spot(there, d, end), stay_sem.at[staying.index(i)])

    def send_targets(late):
        for i, piece in enumerate(pieces):
            if (piece[0] in LATE) != late:
                continue
            if any(piece[3]):

                @pl.when(in_mesh(piece[3]))
                def _(i=i):
                    halo(i).start()

            else:
                stay(i).start()

    load_target.wait()
    send_targets(False)

    inside = {}
    for axis in range(3):
        length = devices[axis] * bricks[axis]
        for place in range(bricks[axis]):
            for step in (-1, 1):
                ahead = at[axis] * bricks[axis] + place + step
                inside[axis, place, step] = ((ahead >= 0) & (ahead < length)).astype(jnp.int32)

    for copy in small:
        copy.wait()
    rows = chunks * side_z
    sub = lax.broadcasted_iota(jnp.int32, (rows, LANES), 0)
    lane = lax.broadcasted_iota(jnp.int32, (rows, LANES), 1)
    point = lane + LANES * (sub // side_z)

    def live_weight(d, y):
        limit = None
        for z in range(side_z):
            value = count[y, z, d] * BLOCK
            for axis, place in enumerate((0, y, z)):
                if OFFSETS[d][axis]:
                    value = value * inside[axis, place, OFFSETS[d][axis]]
            limit = value if limit is None else jnp.where(sub % side_z == z, value, limit)
        return jnp.where(point < limit, own_w[d, y], 0.0)

    for copy in loads:
        copy.wait()
    for y in range(side_y):
        sent_w[y] = live_weight(FLIPPED, y)

    def flip(i):
        start, end = (
            (own_p.at[:, FLIPPED], flip_p),
            (own_n.at[:, FLIPPED], flip_n),
            (sent_w, flip_w),
        )[i]
        return pltpu.make_async_remote_copy(
            src_ref=start,
            dst_ref=end,
            send_sem=flip_send.at[i],
            recv_sem=flip_recv.at[i],
            device_id=beside((1, 0, 0)),
            device_id_type=MESH,
        )

    @pl.when(at_x < count_x - 1)
    def _():
        for i in range(3):
            flip(i).start()

    own_q_rows = own_q.reshape(3, DIRS, side_y, rows, LANES)

    def local(c, d, y):
        return own_q_rows[c, d, y] if d == FLIPPED else own_p[c, d, y]

    def ahead_of(c, d, y):
        return flip_p[c, y] if d == FLIPPED else there_rows[c, d, y]

    def normal_of(c, d, y):
        return flip_n[c, y] if d == FLIPPED else own_n[c, d, y]

    def weight_of(d, y):
        return flip_w[y] if d == FLIPPED else live_weight(d, y)

    def turn(parts):
        missing = LANES - rows * len(parts)
        if missing:
            parts = parts + [jnp.zeros((missing, LANES), jnp.float32)]
        return jnp.concatenate(parts, axis=0).T

    step = 32

    def summed(g, kinds):
        def body(chunk, carry):
            spots = pl.ds(pl.multiple_of(chunk * step, step), step)
            p = [turned[c, g, spots, :] for c in range(3)] + [None]
            q = [turned[7 + c, g, spots, :] for c in range(3)] + [None] if kinds == "there" else None
            n = [turned[3 + c, g, spots, :] for c in range(3)]
            w = turned[6, g, spots, :]

            def times(left, right):
                if left is None:
                    return right
                return left if right is None else left * right

            def add(row, value):
                acc[g, row] += jnp.sum(value.reshape(step // 8, 8, LANES), axis=0)

            wn = [w * n[c] for c in range(3)]
            weighted = [wn[c] * n[k] for c, k in NORMAL_PAIRS]
            if kinds == "here":
                for e in range(4):
                    for s in range(6):
                        add(s * 16 + e * 4 + 3, times(weighted[s], p[e]))
                for place, (e, k) in enumerate(POINT_PAIRS):
                    product = p[e] * p[k]
                    for s in range(6):
                        add(PAIR_ROWS + THERE_ROWS + s * 6 + place, weighted[s] * product)
            else:
                for e in range(4):
                    for k in range(3):
                        product = times(p[e], q[k])
                        for s in range(6):
                            add(s * 16 + e * 4 + k, weighted[s] * product)
                for place, (e, k) in enumerate(POINT_PAIRS):
                    product = q[e] * q[k]
                    for s in range(6):
                        add(PAIR_ROWS + s * 6 + place, weighted[s] * product)
            return carry

        lax.fori_loop(0, LANES // step, body, 0)

    def here(g):
        group = GROUPS[g]
        if FLIPPED in group:

            @pl.when(at_x > 0)
            def _():
                for i in range(3):
                    flip(i).wait_recv()

        for c in range(3):
            turned[c, g] = turn([local(c, d, y) for d in group for y in range(side_y)])
            turned[3 + c, g] = turn([normal_of(c, d, y) for d in group for y in range(side_y)])
        turned[6, g] = turn([weight_of(d, y) for d in group for y in range(side_y)])
        summed(g, "here")

    there_rows = there.reshape(3, DIRS, side_y, rows, LANES)
    last = [None] * side_y
    mine = out.at[at_z, at_x, at_y]

    def tiles_of(values):
        result = values[0]
        for y in range(1, side_y):
            result = jnp.where(sub // side_z == y, values[y], result)
        return result

    def there_sums(g):
        group = GROUPS[g]
        for place, ((of, step), size) in enumerate(arrive.items()):
            if of == g:

                @pl.when(in_mesh(tuple(-s for s in step)))
                def _(place=place, size=size, step=step):
                    halo_bytes(size, 0, place, step).wait_recv()

        for i, piece in enumerate(pieces):
            if piece[0] in group and not any(piece[3]):
                stay(i).wait()
        for c in range(3):
            turned[7 + c, g] = turn([ahead_of(c, d, y) for d in group for y in range(side_y)])
        summed(g, "there")
        whole = [jnp.sum(acc[g, r : r + 8], axis=1) for r in range(0, SUMS, 8)]
        main = jnp.concatenate(whole[: LANES // 8], axis=0).T
        rest = whole[LANES // 8 :] + [jnp.zeros((2 * LANES - SUMS, LANES), jnp.float32)]
        rest = jnp.concatenate(rest, axis=0).T

        def all_chunks(value):
            span = rows // 2
            while span >= side_z:
                value = value + pltpu.roll(value, span, 0)
                span //= 2
            return value

        for place, d in enumerate(group):
            main_rows = []
            for y in range(side_y):
                first = (place * side_y + y) * rows
                main_rows.append(all_chunks(main[first : first + rows]))
                value = all_chunks(rest[first : first + rows])
                spill = pltpu.roll(jnp.where(lane < SPILL, value, 0.0), SPILL_LANE + SPILL * d, 1)
                value = jnp.where(lane < SPILL, 0.0, value) + spill
                last[y] = value if last[y] is None else last[y] + value
            mine[ROW_OF[d]] = tiles_of(main_rows)
        if g < len(GROUPS) - 1:
            return
        pad = [jnp.zeros((rows, AFFINE_LANE), jnp.float32)]
        pad.append(jnp.concatenate([affine[y] for y in range(side_y)], axis=0))
        pad.append(jnp.zeros((rows, LANES - AFFINE_LANE - affine.shape[2]), jnp.float32))
        mine[DIRS] = tiles_of(last) + jnp.concatenate(pad, axis=1)

    everyone = pl.ds(0, count_x)
    halves = (pl.ds(0, count_x // 2), pl.ds(count_x // 2, count_x - count_x // 2))

    def send(c, x, y, z, send_sem, recv_sem, other):
        first, end = CHUNKS[c]
        part = out.at[z, x, y, pl.ds(first, end - first)]
        return pltpu.make_async_remote_copy(
            src_ref=part,
            dst_ref=part,
            send_sem=send_sem,
            recv_sem=recv_sem,
            device_id=other,
            device_id_type=MESH,
        )

    def along(c, step):
        other = (jnp.clip(at_x + step, 0, count_x - 1), at_y, at_z)
        return send(c, at_x, at_y, at_z, sent.at[0], line_recv.at[c, at_x], other)

    def along_in(c, x):
        return send(c, x, at_y, at_z, sent.at[0], line_recv.at[c, x], (x, at_y, at_z))

    def across(c, x, way):
        other = (at_x, near_y[way], at_z)
        return send(c, x, at_y, at_z, sent.at[1], side_recv.at[c, way], other)

    def across_in(c, way):
        other = (at_x, near_y[way], at_z)
        return send(c, everyone, near_y[way], at_z, sent.at[1], side_recv.at[c, way], other)

    def relay(c, way):
        other = (at_x, near_y[1 - way], at_z)
        sems = sent.at[3 + way], side_recv.at[c, 2 + way]
        return send(c, halves[way], near_y[way], at_z, *sems, other)

    def relay_in(c, way):
        other = (at_x, near_y[1 - way], at_z)
        sems = sent.at[3 + way], side_recv.at[c, 2 + way]
        return send(c, halves[way], near_y[2], at_z, *sems, other)

    def core_out(c, x, y, k):
        other = (at_x, at_y, (at_z + k) % count_z)
        return send(c, x, y, at_z, sent.at[2], core_recv.at[c, k - 1], other)

    def core_all(c, z, k):
        other = (at_x, at_y, (at_z + k) % count_z)
        every_y = pl.ds(0, count_y)
        return send(c, everyone, every_y, z, sent.at[2], core_recv.at[c, k - 1], other)

    def to_cores(c, x, y):
        for k in range(1, count_z):
            core_out(c, x, y, k).start()

    def spread(c, x):
        for way in (2, 0, 1) if c in DIRECT else (0, 1):
            across(c, x, way).start()
        to_cores(c, x, at_y)

    far_first = [k for far in range(count_x - 1, 0, -1) for k in (far, -far)]

    def others(body):
        for step in far_first[::-1]:

            @pl.when((at_x + step >= 0) & (at_x + step < count_x))
            def _(step=step):
                body(step)

    def line(c):
        for step in far_first:

            @pl.when((at_x + step >= 0) & (at_x + step < count_x))
            def _(step=step):
                along(c, step).start()

        spread(c, at_x)

    def side(c):
        def body(step):
            along_in(c, at_x + step).wait_recv()
            spread(c, at_x + step)

        others(body)

    def far(c):
        for way in range(2):
            across_in(c, way).wait_recv()
            if c not in DIRECT:
                relay(c, way).start()
            to_cores(c, everyone, near_y[way])

    def core(c):
        if c in DIRECT:
            across_in(c, 2).wait_recv()
        else:
            for way in range(2):
                relay_in(c, way).wait_recv()
        to_cores(c, everyone, near_y[2])

    solver = Solver(devices, bricks, blocks, turned_inverse)
    parts = out.reshape(count_z * count_x * count_y, DIRS + 1, 8, LANES)

    def load(c):
        for k in range(1, count_z):
            core_all(c, (at_z + count_z - k) % count_z, k).wait_recv()
        for r in range(*CHUNKS[c]):
            solver.load(parts, r)

    actions = {
        "here": here, "there": there_sums, "line": line, "side": side, "far": far, "core": core,
        "load": load,
    }
    for entry in SCHEDULE:
        if entry == "late":
            send_targets(True)
            continue
        name, g = entry.split()
        actions[name](int(g))

    def all_sent(kind, region):
        pltpu.make_async_remote_copy(
            src_ref=region,
            dst_ref=region,
            send_sem=sent.at[kind],
            recv_sem=core_recv.at[0, 0],
            device_id=(at_x, at_y, (at_z + 1) % count_z),
            device_id_type=MESH,
        ).wait_send()

    assert len(DIRECT) == len(CHUNKS)
    all_sent(0, out.at[at_z, pl.ds(0, count_x - 1), 0])
    all_sent(1, out.at[at_z, :, pl.ds(0, 3)])
    all_sent(2, out.at[pl.ds(0, count_z - 1)])
    for place, ((_, step), size) in enumerate(arrive.items()):

        @pl.when(in_mesh(step))
        def _(place=place, size=size, step=step):
            halo_bytes(size, place, 0, step).wait_send()

    @pl.when(at_x < count_x - 1)
    def _():
        for i in range(3):
            flip(i).wait_send()

    solver.run(anchor, result_out, tiles)


def on_device(source_points, target_points, normals, weights, blocks, affines, anchor):
    bricks = source_points.shape[2:5]
    points = source_points.shape[5]
    devices = tuple(lax.axis_size(name) for name in AXES)
    grid = tuple(devices[axis] * bricks[axis] for axis in range(3))
    span = grid[0] * grid[1] * grid[2]
    chunks = points // LANES
    rows = chunks * bricks[2]
    assert bricks[0] == 1 and rows == 8 and devices[2] % 2 == 0 and devices[1] == 4
    assert bricks[1] * bricks[2] == 8
    assert span % (2 * LANES) == 0 and len(GROUPS[0]) * bricks[1] * rows == LANES

    def split(value):
        lead = value.shape[:-5]
        value = value.reshape(lead + (DIRS, bricks[1], bricks[2], chunks, LANES))
        return jnp.swapaxes(value, -3, -2)

    def filled(value):
        value = split(value)
        return value.reshape(value.shape[:-3] + (rows, LANES))

    params = functools.partial(pltpu.CompilerParams, vmem_limit_bytes=VMEM_BYTES)
    vmem = pl.BlockSpec(memory_space=pltpu.VMEM)
    anywhere = pl.BlockSpec(memory_space=pl.ANY)
    pieces = halo_pieces(bricks)
    remote = sum(any(piece[3]) for piece in pieces)
    dma = pltpu.SemaphoreType.DMA
    groups = len(GROUPS)
    own = (DIRS, bricks[1], rows, LANES)
    result = pl.pallas_call(
        functools.partial(step_kernel, devices, bricks),
        out_shape=jax.ShapeDtypeStruct(bricks[1:] + (24,), jnp.float32),
        in_specs=[anywhere] * 7,
        out_specs=vmem,
        scratch_shapes=[
            pltpu.SMEM((1,), jnp.int32),
            pltpu.SMEM(bricks[1:] + (DIRS,), jnp.int32),
            pltpu.VMEM(bricks[1:] + (12,), jnp.float32),
            pltpu.VMEM(
                (devices[2], devices[0], devices[1], DIRS + 1, 8, LANES), jnp.float32
            ),
            pltpu.VMEM((DIRS + 1, LANES // 4, 8, span // 2), jnp.float32),
            pltpu.VMEM((36, 8, span // 2), jnp.float32),
            pltpu.VMEM((span // 2, LANES), jnp.float32),
            dma((3,)),
            pltpu.VMEM((3, DIRS, bricks[1], chunks, bricks[2], LANES), jnp.float32),
            pltpu.VMEM((3,) + own, jnp.float32),
            pltpu.VMEM((3,) + own, jnp.float32),
            pltpu.VMEM(own, jnp.float32),
            pltpu.VMEM(own[1:], jnp.float32),
            pltpu.VMEM((3,) + own[1:], jnp.float32),
            pltpu.VMEM((3,) + own[1:], jnp.float32),
            pltpu.VMEM(own[1:], jnp.float32),
            pltpu.VMEM((3, DIRS, bricks[1], chunks, bricks[2], LANES), jnp.float32),
            pltpu.VMEM((10, len(GROUPS), LANES, LANES), jnp.float32),
            pltpu.VMEM((len(GROUPS), SUMS, 8, LANES), jnp.float32),
            dma((4,)),
            dma((len(pieces) - remote,)),
            dma((len(arrivals(pieces)),)),
            dma((len(arrivals(pieces)),)),
            dma((3,)),
            dma((3,)),
            dma((3,)),
            dma((groups, devices[0])),
            dma((groups, 3)),
            dma((groups, devices[2] - 1)),
        ],
        compiler_params=params(collective_id=0, has_side_effects=True),
        name="step",
    )(
        anchor,
        jnp.transpose(blocks, (1, 2, 3, 0)).reshape(bricks[1], bricks[2], DIRS),
        jnp.transpose(affines, (1, 2, 3, 0)).reshape(bricks[1], bricks[2], 12),
        filled(source_points),
        split(target_points),
        filled(normals),
        filled(weights),
    )
    def placed(value):
        return jnp.transpose(value, (2, 0, 1)).reshape((12,) + bricks)

    return placed(result[..., :12]), placed(result[..., 12:])


def solution(mesh):
    points = P(None, None, "gx", "gy", "gz", None)
    tiles = P(None, "gx", "gy", "gz")
    return jax.shard_map(
        on_device,
        mesh=mesh,
        in_specs=(points, points, points, P(None, "gx", "gy", "gz", None), tiles, tiles, P()),
        out_specs=(tiles, tiles),
        check_vma=False,
    )
```
